128 devices in a mesh: row: 8 (over x, core), col: 16 (over y, z).
Axes of the slice: x: 4, y: 4, z: 4, core: 2. Of those that a mesh axis runs over, the one named last changes fastest.
Arguments:
- vectors: float32 [131072, 768], P(('row', 'col')), may hold values from -6 to 6
- list_ids: int32 [131072], P(('row', 'col')), may hold values from 0 to 65535, as said below
- pq_codes: int32 [131072, 96], P(('row', 'col')), may hold values from 0 to 255
- fill_counts: int32 [128, 128], P(('row', 'col')), may hold values from 0 to 8, as said below
- centroids: float32 [65536, 768], P(('row', 'col')), may hold values from -6 to 6
- codebook: float32 [96, 8, 256], P('col'), may hold values from -6 to 6
Outputs:
- coded_err: float32 [131072], P(('row', 'col'))
- best_err: float32 [131072], P(('row', 'col'))
The draws below stay inside these ranges and needn't reach their ends.
Inputs may be any that keep to these rules, and one draw needn't show every extreme that they name: `list_ids`: slot s of device p lies in block s // 8, which belongs to owner device s // 8 (devices numbered row-major over row and col); it names a list of that owner, from (s // 8) * 512 to (s // 8 + 1) * 512 - 1. fill_counts[p, d] is the number of live slots at the head of device p's block for owner d; some owner receives 8 live slots from every device.
All inputs are finite; a program needn't handle non-finite values.
Results may differ from the reference program's by a relative error of at most 0.0003.
Values sent between devices are 32-bit elements; how exact they have to be, the bound alone decides.
No kernel may reach another device: no remote copies, remote signals or barrier semaphores. Data moves between devices by JAX's collectives and lax.ppermute only.
A program may use at most 256 MiB of HBM per device.

```python
import jax
import jax.numpy as jnp
from jax import lax

D = 768
SUB = 8
M = 96
K = 256
LISTS_DEV = 512
LISTS = 65536
SLOTS_DEV = 1024
CAP = 8
ROWS = 131072
DEVICES = 128


def draw_list_ids(key, part):
    slot_index = jnp.arange(ROWS, dtype=jnp.int32) % SLOTS_DEV
    owner = slot_index // CAP
    local_list = jax.random.randint(jax.random.fold_in(key, 11), (ROWS,), 0, LISTS_DEV, dtype=jnp.int32)
    return owner * LISTS_DEV + local_list


def draw_fill_counts(key, part):
    key_hot = jax.random.fold_in(key, 21)
    key_fill = jax.random.fold_in(key, 22)
    shuffled = jax.random.permutation(key_hot, DEVICES)
    hot_rank = shuffled < max(1, DEVICES // 16)
    base_fill = jax.random.randint(key_fill, (DEVICES, DEVICES), 0, CAP + 1, dtype=jnp.int32)
    return jnp.where(hot_rank[None, :], CAP, base_fill).astype(jnp.int32)


def place_ends(drawn, rng, low, largest):
    spot = [jax.random.randint(jax.random.fold_in(rng, axis), (), 0, length) for axis, length in enumerate(drawn.shape)]
    main_axis = drawn.shape.index(max(drawn.shape))
    neighbour = spot[:main_axis] + [(spot[main_axis] + 1) % drawn.shape[main_axis]] + spot[main_axis + 1:]
    return drawn.at[tuple(spot)].set(low).at[tuple(neighbour)].set(largest)


def block_scale(rng, shape, split, low, top_value):
    loudness = 1.0
    for dim, blocks in split:
        heights = jax.random.uniform(jax.random.fold_in(jax.random.fold_in(rng, 6), dim), (blocks,), jnp.float32, low / len(split), top_value / len(split))
        loudness = loudness * jnp.repeat(jnp.exp(heights), shape[dim] // blocks).reshape((-1,) + (1,) * (len(shape) - 1 - dim))
    return loudness


def centred(key, shape, deviation, bound, cuts=(), kind=jnp.bfloat16):
    result = jax.random.normal(key, shape, jnp.float32) * deviation
    if len(cuts) > 0:
        result = block_scale(key, shape, cuts, -0.22, 0.18) * result
    return jnp.clip(result, min=-bound, max=bound).astype(kind)


def setup_inputs(seed: int = 0) -> dict:
    streams_of = jax.random.split(jax.random.key(seed), 7)
    return {
        "vectors": centred(streams_of[0], (ROWS, D), 1.0, 6.0, ((0, 128),), jnp.float32),
        "list_ids": draw_list_ids(jax.random.fold_in(streams_of[6], 71), 0),
        "pq_codes": place_ends(jax.random.randint(streams_of[2], (ROWS, M), 0, K), jax.random.fold_in(streams_of[2], 1), 0, K - 1).astype(jnp.int32),
        "fill_counts": draw_fill_counts(jax.random.fold_in(streams_of[6], 71), 0),
        "centroids": centred(streams_of[4], (LISTS, D), 1.0, 6.0, ((0, 128),), jnp.float32),
        "codebook": centred(streams_of[5], (M, SUB, K), 1.0, 6.0, ((0, 16),), jnp.float32),
    }


def block_terms(block_vec, block_codes, codebook, code_norms):
    resid_norms = jnp.sum(block_vec * block_vec, axis=2)
    cross_term = jnp.einsum("bms,msk->bmk", block_vec, codebook, precision=lax.Precision.HIGHEST)
    dist_table = resid_norms[:, :, None] - 2.0 * cross_term + code_norms[None, :, :]
    best_sum = jnp.sum(jnp.min(dist_table, axis=2), axis=1)
    code_index = lax.broadcasted_iota(jnp.int32, dist_table.shape, 2)
    coded_sum = jnp.sum(jnp.where(code_index == block_codes[:, :, None], dist_table, 0.0), axis=(1, 2))
    return jnp.stack([coded_sum, best_sum])


def reference(vectors, list_ids, pq_codes, fill_counts, centroids, codebook):
    device_count = fill_counts.shape[0]
    slot_count = vectors.shape[0] // device_count
    capacity = slot_count // device_count
    sub_count = pq_codes.shape[1]
    sub_width = vectors.shape[1] // sub_count
    block_rows = 256
    block_count = slot_count // block_rows
    code_norms = jnp.sum(codebook * codebook, axis=1)

    def one_device(inputs):
        device_vec, device_ids, device_codes = inputs
        residual = device_vec - jnp.take(centroids, device_ids, axis=0)
        shaped = residual.reshape(block_count, block_rows, sub_count, sub_width)
        shaped_codes = device_codes.reshape(block_count, block_rows, sub_count)

        def one_block(pair):
            return block_terms(pair[0], pair[1], codebook, code_norms)

        parts = lax.map(one_block, (shaped, shaped_codes))
        return jnp.transpose(parts, (1, 0, 2)).reshape(2, slot_count)

    results = lax.map(one_device, (vectors.reshape(device_count, slot_count, -1), list_ids.reshape(device_count, slot_count), pq_codes.reshape(device_count, slot_count, sub_count)))
    slot_pos = jnp.arange(capacity, dtype=jnp.int32)
    live_mask = (slot_pos[None, None, :] < fill_counts[:, :, None]).reshape(device_count, slot_count)
    coded_err = jnp.where(live_mask, results[:, 0, :], 0.0).reshape(-1)
    best_err = jnp.where(live_mask, results[:, 1, :], 0.0).reshape(-1)
    return coded_err, best_err
```

```python
import functools

import jax
import jax.numpy as jnp
from jax import lax
from jax.experimental import pallas as pl
from jax.experimental.pallas import tpu as pltpu
from jax.sharding import PartitionSpec as P

BOTH = ("row", "col")
LANES = 128
SPLITS = 64


def three_way(x):
    hi = x.astype(jnp.bfloat16).astype(jnp.float32)
    rest = x - hi
    mid = rest.astype(jnp.bfloat16).astype(jnp.float32)
    lo = (rest - mid).astype(jnp.bfloat16).astype(jnp.float32)
    return hi, mid, lo


def prep_kernel(core_ref, vec_ref, codes_ref, own_ref, sib_ref, vt_ref, wt_ref, a_ref):
    step = pl.program_id(0)
    core = core_ref[0]
    rows = vec_ref.shape[0]
    sublane = lax.broadcasted_iota(jnp.int32, (8, 256), 0)
    lane = lax.broadcasted_iota(jnp.int32, (256, LANES), 1)
    for g in range(rows // LANES):
        vt_ref[:, g * LANES : (g + 1) * LANES] = vec_ref[g * LANES : (g + 1) * LANES, :].T
    stacks = []
    for i in range(16):
        m = step * 16 + i
        shard, within = m // 6, m % 6
        half, j = within // 3, within % 3
        base = shard * 8 + j * 2
        mine = half == core
        words = []
        for h in range(2):
            spot = pl.ds(base + h, 8, stride=LANES)
            words.append(jnp.where(mine, own_ref[spot, :], sib_ref[spot, :]))
        for g in range(rows // LANES):
            cut = slice(g * LANES, (g + 1) * LANES)
            code = jnp.broadcast_to(codes_ref[i : i + 1, cut], (8, LANES))
            low = code & (LANES - 1)
            first = jnp.take_along_axis(words[0], low, axis=1, mode="promise_in_bounds")
            second = jnp.take_along_axis(words[1], low, axis=1, mode="promise_in_bounds")
            word = jnp.where(code >= LANES, second, first)
            wt_ref[i * 8 : (i + 1) * 8, cut] = vt_ref[i * 8 : (i + 1) * 8, cut] - word
        both = jnp.concatenate(words, axis=1)
        norm = jnp.sum(both * both, axis=0, keepdims=True)
        hi, mid, lo = three_way(-2.0 * both)
        nhi, nmid, nlo = three_way(norm)
        norms = jnp.where(sublane == 0, nhi, jnp.where(sublane == 1, nmid, jnp.where(sublane == 2, nlo, 0.0)))
        stacks.append([hi, hi, hi, mid, mid, lo, norms, jnp.zeros_like(norms)])
        if i % 2 == 1:
            turned = jnp.concatenate(stacks[0] + stacks[1], axis=0).T
            a_ref[i - 1] = jnp.where(lane < SPLITS, turned, 0.0).astype(jnp.bfloat16)
            a_ref[i] = jnp.where(lane < SPLITS, 0.0, turned).astype(jnp.bfloat16)
            stacks = []


def score_kernel(vt_ref, wt_ref, cent_ref, a_ref, live_ref, coded_ref, best_ref, acc_ref):
    step = pl.program_id(0)
    rows = cent_ref.shape[0]
    wide = 256

    @pl.when(step == 0)
    def _():
        acc_ref[...] = jnp.zeros_like(acc_ref)

    ones = jnp.ones((16, wide), jnp.bfloat16)
    for t in range(rows // wide):
        cut = slice(t * wide, (t + 1) * wide)
        turned = jnp.concatenate(
            [cent_ref[t * wide + g * LANES : t * wide + (g + 1) * LANES, :].T for g in range(wide // LANES)],
            axis=1,
        )
        resid = vt_ref[:, cut] - turned
        err = wt_ref[:, cut] - turned
        acc_ref[0:8, cut] += jnp.sum((err * err).reshape(16, 8, wide), axis=0)
        acc_ref[8:16, cut] += jnp.sum((resid * resid).reshape(16, 8, wide), axis=0)
        least = jnp.zeros((1, wide), jnp.float32)
        for pair in range(8):
            side = []
            for half in range(2):
                at = (pair * 2 + half) * 8
                hi, mid, lo = three_way(resid[at : at + 8, :])
                side += [
                    jnp.concatenate([hi, mid], axis=0).astype(jnp.bfloat16),
                    jnp.concatenate([lo, hi], axis=0).astype(jnp.bfloat16),
                    jnp.concatenate([mid, hi], axis=0).astype(jnp.bfloat16),
                    ones,
                ]
            right = jnp.concatenate(side, axis=0)
            for half in range(2):
                table = jnp.dot(a_ref[pair * 2 + half], right, preferred_element_type=jnp.float32)
                least += jnp.min(table, axis=0, keepdims=True)
        acc_ref[16:17, cut] += least

    @pl.when(step == pl.num_programs(0) - 1)
    def _():
        live = live_ref[...] != 0
        coded = jnp.sum(acc_ref[0:8, :], axis=0, keepdims=True)
        best = jnp.sum(acc_ref[8:16, :], axis=0, keepdims=True) + acc_ref[16:17, :]
        coded_ref[...] = jnp.where(live, coded, 0.0)
        best_ref[...] = jnp.where(live, best, 0.0)


def local(vectors, list_ids, pq_codes, fill_counts, centroids, codebook):
    row_count = lax.axis_size("row")
    col_count = lax.axis_size("col")
    devices = row_count * col_count
    slots, width = vectors.shape
    cap = slots // devices
    subs = pq_codes.shape[1]
    f32 = jnp.float32
    my_row = lax.axis_index("row")
    core = my_row % 2

    coord = lax.dynamic_index_in_dim(codebook, my_row, axis=1, keepdims=False)
    halves = coord.reshape(2, 6, LANES)
    piece = jnp.broadcast_to(halves[None, :, None], (row_count // 2, 2, col_count, 6, LANES))
    piece = piece.reshape(devices, 6, LANES)
    ids = (list_ids.reshape(devices, 1, cap) % centroids.shape[0]).astype(f32)
    ids = jnp.pad(ids, ((0, 0), (0, 1), (0, LANES - cap)))
    sent = jnp.concatenate([piece, ids], axis=1)
    got = lax.all_to_all(sent, BOTH, 0, 0, tiled=True)
    sibling = lax.ppermute(got, "row", [(i, i ^ 1) for i in range(row_count)])

    want = got[:, 6, :cap].astype(jnp.int32).reshape(slots)
    picked = centroids.at[want].get(mode="promise_in_bounds")
    cent = lax.all_to_all(picked.reshape(devices, cap, width), BOTH, 0, 0, tiled=True)
    cent = cent.reshape(slots, width)

    steps = width // LANES
    per = subs // steps
    vt, wt, a = pl.pallas_call(
        prep_kernel,
        grid=(steps,),
        in_specs=[
            pl.BlockSpec(memory_space=pltpu.SMEM),
            pl.BlockSpec((slots, LANES), lambda i: (0, i)),
            pl.BlockSpec((per, slots), lambda i: (i, 0)),
            pl.BlockSpec((devices * 8, LANES), lambda i: (0, 0)),
            pl.BlockSpec((devices * 8, LANES), lambda i: (0, 0)),
        ],
        out_specs=[
            pl.BlockSpec((LANES, slots), lambda i: (i, 0)),
            pl.BlockSpec((LANES, slots), lambda i: (i, 0)),
            pl.BlockSpec((per, 256, LANES), lambda i: (i, 0, 0)),
        ],
        out_shape=[
            jax.ShapeDtypeStruct((width, slots), f32),
            jax.ShapeDtypeStruct((width, slots), f32),
            jax.ShapeDtypeStruct((subs, 256, LANES), jnp.bfloat16),
        ],
        name="prep",
    )(
        core.reshape(1).astype(jnp.int32),
        vectors,
        pq_codes.T,
        got.reshape(devices * 8, LANES),
        sibling.reshape(devices * 8, LANES),
    )

    slot_pos = jnp.arange(cap, dtype=jnp.int32)
    live = (slot_pos[None, :] < fill_counts[0][:, None]).astype(jnp.int32).reshape(1, slots)
    coded, best = pl.pallas_call(
        score_kernel,
        grid=(steps,),
        in_specs=[
            pl.BlockSpec((LANES, slots), lambda i: (i, 0)),
            pl.BlockSpec((LANES, slots), lambda i: (i, 0)),
            pl.BlockSpec((slots, LANES), lambda i: (0, i)),
            pl.BlockSpec((per, 256, LANES), lambda i: (i, 0, 0)),
            pl.BlockSpec((1, slots), lambda i: (0, 0)),
        ],
        out_specs=[pl.BlockSpec((1, slots), lambda i: (0, 0))] * 2,
        out_shape=[jax.ShapeDtypeStruct((1, slots), f32)] * 2,
        scratch_shapes=[pltpu.VMEM((24, slots), f32)],
        name="score",
    )(vt, wt, cent, a, live)
    return coded.reshape(slots), best.reshape(slots)


def solution(mesh):
    in_specs = (
        P(BOTH, None),
        P(BOTH),
        P(BOTH, None),
        P(BOTH, None),
        P(BOTH, None),
        P("col", None, None),
    )
    out_specs = (P(BOTH), P(BOTH))
    return jax.shard_map(local, mesh=mesh, in_specs=in_specs, out_specs=out_specs, check_vma=False)
```

```python
import jax
import jax.numpy as jnp
from jax import lax
from jax.experimental import pallas as pl
from jax.experimental.pallas import tpu as pltpu
from jax.sharding import PartitionSpec as P

BOTH = ("row", "col")
LANES = 128
SPLITS = 64


def three_way(x):
    hi = x.astype(jnp.bfloat16).astype(jnp.float32)
    rest = x - hi
    mid = rest.astype(jnp.bfloat16).astype(jnp.float32)
    lo = (rest - mid).astype(jnp.bfloat16).astype(jnp.float32)
    return hi, mid, lo


def prep_kernel(core_ref, vec_ref, codes_ref, own_ref, sib_ref, vt_ref, wt_ref, a_ref):
    core = core_ref[0]
    rows, width = vec_ref.shape
    sublane = lax.broadcasted_iota(jnp.int32, (8, 256), 0)
    for block in range(width // LANES):
        for g in range(rows // LANES):
            vt_ref[block * LANES : (block + 1) * LANES, g * LANES : (g + 1) * LANES] = vec_ref[
                g * LANES : (g + 1) * LANES, block * LANES : (block + 1) * LANES
            ].T

    def some_subspaces(step, carry):
        codes = codes_ref[pl.ds(pl.multiple_of(step * 8, 8), 8), :]
        stack = []
        for i in range(8):
            m = step * 8 + i
            shard, within = m // 6, m % 6
            half, j = within // 3, within % 3
            base = shard * 8 + j * 2
            mine = half == core
            words = []
            for h in range(2):
                spot = pl.ds(base + h, 8, stride=LANES)
                words.append(jnp.where(mine, own_ref[spot, :], sib_ref[spot, :]))
            at = pl.ds(pl.multiple_of(m * 8, 8), 8)
            for g in range(rows // LANES):
                cut = slice(g * LANES, (g + 1) * LANES)
                code = jnp.broadcast_to(codes[i : i + 1, cut], (8, LANES))
                low = code & (LANES - 1)
                first = jnp.take_along_axis(words[0], low, axis=1, mode="promise_in_bounds")
                second = jnp.take_along_axis(words[1], low, axis=1, mode="promise_in_bounds")
                wt_ref[at, cut] = vt_ref[at, cut] - jnp.where(code >= LANES, second, first)
            both = jnp.concatenate(words, axis=1)
            norm = jnp.sum(both * both, axis=0, keepdims=True)
            hi, mid, lo = three_way(-2.0 * both)
            nhi, nmid, nlo = three_way(norm)
            norms = jnp.where(sublane == 0, nhi, jnp.where(sublane == 1, nmid, jnp.where(sublane == 2, nlo, 0.0)))
            stack += [hi, hi, hi, mid, mid, lo, norms, jnp.zeros_like(norms)]
            if i % 2 == 1:
                a_ref[m // 2] = jnp.concatenate(stack, axis=0).T.astype(jnp.bfloat16)
                stack = []
        return carry

    lax.fori_loop(0, codes_ref.shape[0] // 8, some_subspaces, 0)


PARTS = 8


def pick_kernel(start_ref, cent_ref, out_hbm, out_ref, sems):
    tiles = 6
    words = out_ref.shape[0] // PARTS
    slots = words // tiles
    copies = []
    for part in range(PARTS):

        def some(i, carry, part=part):
            for k in range(32):
                row = cent_ref[pl.ds(start_ref[part * slots + i * 32 + k], tiles, stride=8), :]
                out_ref[pl.ds(part * words + (i * 4 + k // 8) * (8 * tiles) + k % 8, tiles, stride=8), :] = row
            return carry

        lax.fori_loop(0, slots // 32, some, 0)
        cut = slice(part * words, (part + 1) * words)
        copies.append(pltpu.make_async_copy(out_ref.at[cut], out_hbm.at[cut], sems.at[part]))
        copies[-1].start()
    for copy in copies:
        copy.wait()


def tiled_view(x):
    n, w = x.shape
    return x.reshape(n // 8, 8, w // LANES, LANES).swapaxes(1, 2).reshape(n * w // LANES, LANES)


def untiled_view(x, n, w):
    return x.reshape(n // 8, w // LANES, 8, LANES).swapaxes(1, 2).reshape(n, w)


STAGES = ((0, 1), (1, 3), (3, 6))


def score_kernel(vt_hbm, wt_hbm, cent_ref, a_hbm, live_ref, coded_ref, best_ref, vt_ref, wt_ref, a_ref, acc_ref, sems):
    rows, width = cent_ref.shape
    wide = 256
    tiles = rows // wide
    copies = []
    for k, (lo, hi) in enumerate(STAGES):
        pairs = slice(lo * 8, hi * 8)
        feats = slice(lo * LANES, hi * LANES)
        copies.append(
            [
                pltpu.make_async_copy(a_hbm.at[pairs], a_ref.at[pairs], sems.at[k, 0]),
                pltpu.make_async_copy(vt_hbm.at[feats], vt_ref.at[feats], sems.at[k, 1]),
                pltpu.make_async_copy(wt_hbm.at[feats], wt_ref.at[feats], sems.at[k, 2]),
            ]
        )
        for copy in copies[-1]:
            copy.start()
    acc_ref[...] = jnp.zeros_like(acc_ref)
    ones = jnp.ones((16, wide), jnp.bfloat16)
    none = jnp.zeros((SPLITS, wide), jnp.bfloat16)
    for k, (lo, hi) in enumerate(STAGES):
        for copy in copies[k]:
            copy.wait()
        for block in range(lo, hi):
            feats = slice(block * LANES, (block + 1) * LANES)
            for t in range(tiles):
                cut = slice(t * wide, (t + 1) * wide)
                turned = jnp.concatenate(
                    [
                        cent_ref[t * wide + g * LANES : t * wide + (g + 1) * LANES, feats].T
                        for g in range(wide // LANES)
                    ],
                    axis=1,
                )
                resid = vt_ref[feats, cut] - turned
                err = wt_ref[feats, cut] - turned
                least = jnp.zeros((1, wide), jnp.float32)
                for pair in range(8):
                    left = a_ref[block * 8 + pair]
                    for half in range(2):
                        at = (pair * 2 + half) * 8
                        hi_, mid, low = three_way(resid[at : at + 8, :])
                        side = [
                            jnp.concatenate([hi_, mid], axis=0).astype(jnp.bfloat16),
                            jnp.concatenate([low, hi_], axis=0).astype(jnp.bfloat16),
                            jnp.concatenate([mid, hi_], axis=0).astype(jnp.bfloat16),
                            ones,
                        ]
                        side = [none] + side if half else side + [none]
                        table = jnp.dot(left, jnp.concatenate(side, axis=0), preferred_element_type=jnp.float32)
                        least += jnp.min(table, axis=0, keepdims=True)
                acc_ref[0:8, cut] += jnp.sum((err * err).reshape(16, 8, wide), axis=0)
                acc_ref[8:16, cut] += jnp.sum((resid * resid).reshape(16, 8, wide), axis=0)
                acc_ref[16:17, cut] += least
    live = live_ref[...] != 0
    coded = jnp.sum(acc_ref[0:8, :], axis=0, keepdims=True)
    best = jnp.sum(acc_ref[8:16, :], axis=0, keepdims=True) + acc_ref[16:17, :]
    coded_ref[...] = jnp.where(live, coded, 0.0)
    best_ref[...] = jnp.where(live, best, 0.0)


def pinned(x):
    return pltpu.with_memory_space_constraint(x, pltpu.HBM)


def local(vectors, list_ids, pq_codes, fill_counts, centroids, codebook):
    row_count = lax.axis_size("row")
    col_count = lax.axis_size("col")
    devices = row_count * col_count
    slots, width = vectors.shape
    cap = slots // devices
    subs = pq_codes.shape[1]
    f32 = jnp.float32
    my_row = lax.axis_index("row")
    core = my_row % 2

    coord = lax.dynamic_index_in_dim(codebook, my_row, axis=1, keepdims=False)
    halves = coord.reshape(2, 6, LANES)
    piece = jnp.broadcast_to(halves[None, :, None], (row_count // 2, 2, col_count, 6, LANES))
    piece = piece.reshape(devices, 6, LANES)
    per_row = LANES // cap
    ids = list_ids.astype(f32).reshape(devices // per_row, 1, 1, LANES)
    ids = jnp.broadcast_to(ids, (devices // per_row, per_row, 2, LANES)).reshape(devices, 2, LANES)
    sent = jnp.concatenate([piece, ids], axis=1)
    got = lax.all_to_all(sent, BOTH, 0, 0, tiled=True)
    sibling = lax.ppermute(got, "row", [(i, i ^ 1) for i in range(row_count)])

    me = my_row * col_count + lax.axis_index("col")
    want = lax.dynamic_slice(got[:, 6], (0, (me % per_row) * cap), (devices, cap))
    want = want.astype(jnp.int32).reshape(slots) % centroids.shape[0]
    start = (want // 8) * (8 * width // LANES) + want % 8
    vmem = pl.BlockSpec(memory_space=pltpu.VMEM)
    smem = pl.BlockSpec(memory_space=pltpu.SMEM)
    hbm = pl.BlockSpec(memory_space=pltpu.HBM)
    picked = pl.pallas_call(
        pick_kernel,
        in_specs=[smem, vmem],
        out_specs=hbm,
        out_shape=pltpu.HBM((slots * width // LANES, LANES), f32),
        scratch_shapes=[pltpu.VMEM((slots * width // LANES, LANES), f32), pltpu.SemaphoreType.DMA((PARTS,))],
        compiler_params=pltpu.CompilerParams(vmem_limit_bytes=8 << 20),
        name="pick",
    )(start, tiled_view(centroids))
    picked = untiled_view(picked, slots, width)
    cent = lax.all_to_all(picked.reshape(devices, cap, width), BOTH, 0, 0, tiled=True)
    cent = cent.reshape(slots, width)

    vt, wt, a = pl.pallas_call(
        prep_kernel,
        in_specs=[smem, vmem, vmem, vmem, vmem],
        out_specs=[vmem] * 3,
        out_shape=[
            jax.ShapeDtypeStruct((width, slots), f32),
            jax.ShapeDtypeStruct((width, slots), f32),
            jax.ShapeDtypeStruct((subs // 2, 256, LANES), jnp.bfloat16),
        ],
        compiler_params=pltpu.CompilerParams(vmem_limit_bytes=24 << 20),
        name="prep",
    )(
        core.reshape(1).astype(jnp.int32),
        vectors,
        pq_codes.T,
        got.reshape(devices * 8, LANES),
        sibling.reshape(devices * 8, LANES),
    )

    slot_pos = jnp.arange(cap, dtype=jnp.int32)
    live = (slot_pos[None, :] < fill_counts[0][:, None]).astype(jnp.int32).reshape(1, slots)
    coded, best = pl.pallas_call(
        score_kernel,
        in_specs=[hbm, hbm, vmem, hbm, vmem],
        out_specs=[vmem] * 2,
        out_shape=[jax.ShapeDtypeStruct((1, slots), f32)] * 2,
        scratch_shapes=[
            pltpu.VMEM((width, slots), f32),
            pltpu.VMEM((width, slots), f32),
            pltpu.VMEM((subs // 2, 256, LANES), jnp.bfloat16),
            pltpu.VMEM((24, slots), f32),
            pltpu.SemaphoreType.DMA((len(STAGES), 3)),
        ],
        compiler_params=pltpu.CompilerParams(vmem_limit_bytes=32 << 20),
        name="score",
    )(pinned(vt), pinned(wt), cent, pinned(a), live)
    return coded.reshape(slots), best.reshape(slots)


def solution(mesh):
    in_specs = (
        P(BOTH, None),
        P(BOTH),
        P(BOTH, None),
        P(BOTH, None),
        P(BOTH, None),
        P("col", None, None),
    )
    out_specs = (P(BOTH), P(BOTH))
    return jax.shard_map(local, mesh=mesh, in_specs=in_specs, out_specs=out_specs, check_vma=False)
```

```python
import jax
import jax.numpy as jnp
from jax import lax
from jax.experimental import pallas as pl
from jax.experimental.pallas import tpu as pltpu
from jax.sharding import PartitionSpec as P

BOTH = ("row", "col")
LANES = 128
SPLITS = 64


def three_way(x):
    hi = x.astype(jnp.bfloat16).astype(jnp.float32)
    rest = x - hi
    mid = rest.astype(jnp.bfloat16).astype(jnp.float32)
    lo = (rest - mid).astype(jnp.bfloat16).astype(jnp.float32)
    return hi, mid, lo


def prep_kernel(spot_ref, vec_ref, codes_ref, book_ref, vt_ref, wt_ref, a_ref):
    rows, width = vec_ref.shape
    sublane = lax.broadcasted_iota(jnp.int32, (8, 256), 0)
    for block in range(width // LANES):
        for g in range(rows // LANES):
            vt_ref[block * LANES : (block + 1) * LANES, g * LANES : (g + 1) * LANES] = vec_ref[
                g * LANES : (g + 1) * LANES, block * LANES : (block + 1) * LANES
            ].T

    def some_subspaces(step, carry):
        codes = codes_ref[pl.ds(pl.multiple_of(step * 8, 8), 8), :]
        stack = []
        for i in range(8):
            m = step * 8 + i
            at = pl.multiple_of((spot_ref[m // 6] * 6 + m % 6) * 8, 8)
            both = book_ref[pl.ds(at, 8), :]
            words = [both[:, :LANES], both[:, LANES:]]
            at = pl.ds(pl.multiple_of(m * 8, 8), 8)
            for g in range(rows // LANES):
                cut = slice(g * LANES, (g + 1) * LANES)
                code = jnp.broadcast_to(codes[i : i + 1, cut], (8, LANES))
                low = code & (LANES - 1)
                first = jnp.take_along_axis(words[0], low, axis=1, mode="promise_in_bounds")
                second = jnp.take_along_axis(words[1], low, axis=1, mode="promise_in_bounds")
                wt_ref[at, cut] = vt_ref[at, cut] - jnp.where(code >= LANES, second, first)
            norm = jnp.sum(both * both, axis=0, keepdims=True)
            hi, mid, lo = three_way(-2.0 * both)
            nhi, nmid, nlo = three_way(norm)
            norms = jnp.where(sublane == 0, nhi, jnp.where(sublane == 1, nmid, jnp.where(sublane == 2, nlo, 0.0)))
            stack += [hi, hi, hi, mid, mid, lo, norms, jnp.zeros_like(norms)]
            if i % 2 == 1:
                a_ref[m // 2] = jnp.concatenate(stack, axis=0).T.astype(jnp.bfloat16)
                stack = []
        return carry

    lax.fori_loop(0, codes_ref.shape[0] // 8, some_subspaces, 0)


PARTS = 8


def pick_kernel(start_ref, cent_ref, out_hbm, out_ref, sems):
    tiles = 6
    words = out_ref.shape[0] // PARTS
    slots = words // tiles
    copies = []
    for part in range(PARTS):

        def some(i, carry, part=part):
            for k in range(32):
                row = cent_ref[pl.ds(start_ref[part * slots + i * 32 + k], tiles, stride=8), :]
                out_ref[pl.ds(part * words + (i * 4 + k // 8) * (8 * tiles) + k % 8, tiles, stride=8), :] = row
            return carry

        lax.fori_loop(0, slots // 32, some, 0)
        cut = slice(part * words, (part + 1) * words)
        copies.append(pltpu.make_async_copy(out_ref.at[cut], out_hbm.at[cut], sems.at[part]))
        copies[-1].start()
    for copy in copies:
        copy.wait()


def tiled_view(x):
    n, w = x.shape
    return x.reshape(n // 8, 8, w // LANES, LANES).swapaxes(1, 2).reshape(n * w // LANES, LANES)


def untiled_view(x, n, w):
    return x.reshape(n // 8, w // LANES, 8, LANES).swapaxes(1, 2).reshape(n, w)


STAGES = ((0, 1), (1, 3), (3, 6))


def score_kernel(vt_hbm, wt_hbm, cent_ref, a_hbm, live_ref, coded_ref, best_ref, vt_ref, wt_ref, a_ref, acc_ref, sems):
    rows, width = cent_ref.shape
    wide = 256

    def fetch(k):
        lo, hi = STAGES[k]
        pairs, feats = slice(lo * 8, hi * 8), slice(lo * LANES, hi * LANES)
        copies = [
            pltpu.make_async_copy(a_hbm.at[pairs], a_ref.at[pairs], sems.at[k, 0]),
            pltpu.make_async_copy(vt_hbm.at[feats], vt_ref.at[feats], sems.at[k, 1]),
        ]
        if k > 0:
            feats = slice(0 if k == 1 else lo * LANES, hi * LANES)
            copies.append(pltpu.make_async_copy(wt_hbm.at[feats], wt_ref.at[feats], sems.at[k, 2]))
        for copy in copies:
            copy.start()
        return copies

    def turned(block, t):
        spots = [slice(t * wide + g * LANES, t * wide + (g + 1) * LANES) for g in range(wide // LANES)]
        return jnp.concatenate([cent_ref[at, block * LANES : (block + 1) * LANES].T for at in spots], axis=1)

    waiting = [fetch(0)]
    acc_ref[...] = jnp.zeros_like(acc_ref)
    ones = jnp.ones((16, wide), jnp.bfloat16)
    none = jnp.zeros((SPLITS, wide), jnp.bfloat16)
    for k, (lo, hi) in enumerate(STAGES):
        for copy in waiting[k]:
            copy.wait()
        if k == 0:
            waiting += [fetch(j) for j in range(1, len(STAGES))]
        for block in range(lo, hi):
            feats = slice(block * LANES, (block + 1) * LANES)
            for t in range(rows // wide):
                cut = slice(t * wide, (t + 1) * wide)
                cent = turned(block, t)
                resid = vt_ref[feats, cut] - cent
                least = jnp.zeros((1, wide), jnp.float32)
                for pair in range(8):
                    left = a_ref[block * 8 + pair]
                    for half in range(2):
                        at = (pair * 2 + half) * 8
                        top, mid, low = three_way(resid[at : at + 8, :])
                        side = [
                            jnp.concatenate([top, mid], axis=0).astype(jnp.bfloat16),
                            jnp.concatenate([low, top], axis=0).astype(jnp.bfloat16),
                            jnp.concatenate([mid, top], axis=0).astype(jnp.bfloat16),
                            ones,
                        ]
                        side = [none] + side if half else side + [none]
                        table = jnp.dot(left, jnp.concatenate(side, axis=0), preferred_element_type=jnp.float32)
                        least += jnp.min(table, axis=0, keepdims=True)
                acc_ref[8:16, cut] += jnp.sum((resid * resid).reshape(16, 8, wide), axis=0)
                acc_ref[16:17, cut] += least
                if k > 0:
                    err = wt_ref[feats, cut] - cent
                    acc_ref[0:8, cut] += jnp.sum((err * err).reshape(16, 8, wide), axis=0)
                if block == 1:
                    err = wt_ref[0:LANES, cut] - turned(0, t)
                    acc_ref[0:8, cut] += jnp.sum((err * err).reshape(16, 8, wide), axis=0)
    live = live_ref[...] != 0
    coded = jnp.sum(acc_ref[0:8, :], axis=0, keepdims=True)
    best = jnp.sum(acc_ref[8:16, :], axis=0, keepdims=True) + acc_ref[16:17, :]
    coded_ref[...] = jnp.where(live, coded, 0.0)
    best_ref[...] = jnp.where(live, best, 0.0)


SIDE = 4


def moved(x, dy, dz):
    pairs = []
    for y in range(SIDE):
        for z in range(SIDE):
            pairs.append((y * SIDE + z, (y + dy) % SIDE * SIDE + (z + dz) % SIDE))
    return lax.ppermute(x, "col", pairs)


def gathered_book(codebook):
    mine = codebook.reshape(-1, codebook.shape[2])
    with jax.named_scope("book1"):
        back, ahead = moved(mine, 0, 1), moved(mine, 0, -1)
    with jax.named_scope("book2"):
        far = moved(back, 0, 1)
    line = jnp.concatenate([mine, back, ahead, far])
    with jax.named_scope("book3"):
        back, ahead = moved(line, 1, 0), moved(line, -1, 0)
    with jax.named_scope("book4"):
        far = moved(back, 1, 0)
    book = jnp.concatenate([line, back, ahead, far])
    col = lax.axis_index("col")
    shard = jnp.arange(SIDE * SIDE, dtype=jnp.int32)

    def place(theirs, own):
        ahead_by = (theirs - own) % SIDE
        return jnp.where(ahead_by == SIDE - 1, 1, jnp.where(ahead_by == 0, 0, ahead_by + 1))

    spots = place(shard // SIDE, col // SIDE) * SIDE + place(shard % SIDE, col % SIDE)
    return book, spots.astype(jnp.int32)


def pinned(x):
    return pltpu.with_memory_space_constraint(x, pltpu.HBM)


def local(vectors, list_ids, pq_codes, fill_counts, centroids, codebook):
    row_count = lax.axis_size("row")
    col_count = lax.axis_size("col")
    devices = row_count * col_count
    slots, width = vectors.shape
    cap = slots // devices
    subs = pq_codes.shape[1]
    f32 = jnp.float32
    me = lax.axis_index("row") * col_count + lax.axis_index("col")

    per_row = LANES // cap
    ids = jnp.broadcast_to(list_ids.reshape(devices // per_row, 1, 1, LANES), (devices // per_row, per_row, 1, LANES))
    with jax.named_scope("ids"):
        got = lax.all_to_all(ids.reshape(devices, 1, LANES), BOTH, 0, 0, tiled=True)
    want = lax.dynamic_slice(got[:, 0], (0, (me % per_row) * cap), (devices, cap)).reshape(slots)
    want = want % centroids.shape[0]
    start = (want // 8) * (8 * width // LANES) + want % 8
    book, spots = gathered_book(codebook)
    vmem = pl.BlockSpec(memory_space=pltpu.VMEM)
    smem = pl.BlockSpec(memory_space=pltpu.SMEM)
    hbm = pl.BlockSpec(memory_space=pltpu.HBM)
    picked = pl.pallas_call(
        pick_kernel,
        in_specs=[smem, vmem],
        out_specs=hbm,
        out_shape=pltpu.HBM((slots * width // LANES, LANES), f32),
        scratch_shapes=[pltpu.VMEM((slots * width // LANES, LANES), f32), pltpu.SemaphoreType.DMA((PARTS,))],
        compiler_params=pltpu.CompilerParams(vmem_limit_bytes=8 << 20),
        name="pick",
    )(start, tiled_view(centroids))
    picked = untiled_view(picked, slots, width)
    with jax.named_scope("rows"):
        cent = lax.all_to_all(picked.reshape(devices, cap, width), BOTH, 0, 0, tiled=True)
    cent = cent.reshape(slots, width)

    vt, wt, a = pl.pallas_call(
        prep_kernel,
        in_specs=[smem, vmem, vmem, vmem],
        out_specs=[vmem] * 3,
        out_shape=[
            jax.ShapeDtypeStruct((width, slots), f32),
            jax.ShapeDtypeStruct((width, slots), f32),
            jax.ShapeDtypeStruct((subs // 2, 256, LANES), jnp.bfloat16),
        ],
        compiler_params=pltpu.CompilerParams(vmem_limit_bytes=24 << 20),
        name="prep",
    )(
        spots,
        vectors,
        pq_codes.T,
        book,
    )

    slot_pos = jnp.arange(cap, dtype=jnp.int32)
    live = (slot_pos[None, :] < fill_counts[0][:, None]).astype(jnp.int32).reshape(1, slots)
    coded, best = pl.pallas_call(
        score_kernel,
        in_specs=[hbm, hbm, vmem, hbm, vmem],
        out_specs=[vmem] * 2,
        out_shape=[jax.ShapeDtypeStruct((1, slots), f32)] * 2,
        scratch_shapes=[
            pltpu.VMEM((width, slots), f32),
            pltpu.VMEM((width, slots), f32),
            pltpu.VMEM((subs // 2, 256, LANES), jnp.bfloat16),
            pltpu.VMEM((24, slots), f32),
            pltpu.SemaphoreType.DMA((len(STAGES), 3)),
        ],
        compiler_params=pltpu.CompilerParams(vmem_limit_bytes=32 << 20),
        name="score",
    )(pinned(vt), pinned(wt), cent, pinned(a), live)
    return coded.reshape(slots), best.reshape(slots)


def solution(mesh):
    in_specs = (
        P(BOTH, None),
        P(BOTH),
        P(BOTH, None),
        P(BOTH, None),
        P(BOTH, None),
        P("col", None, None),
    )
    out_specs = (P(BOTH), P(BOTH))
    return jax.shard_map(local, mesh=mesh, in_specs=in_specs, out_specs=out_specs, check_vma=False)
```

```python
import jax
import jax.numpy as jnp
from jax import lax
from jax.experimental import pallas as pl
from jax.experimental.pallas import tpu as pltpu
from jax.sharding import PartitionSpec as P

BOTH = ("row", "col")
LANES = 128
SPLITS = 64


def three_way(x):
    hi = x.astype(jnp.bfloat16).astype(jnp.float32)
    rest = x - hi
    mid = rest.astype(jnp.bfloat16).astype(jnp.float32)
    lo = (rest - mid).astype(jnp.bfloat16).astype(jnp.float32)
    return hi, mid, lo


def prep_kernel(core_ref, vec_ref, codes_ref, own_ref, sib_ref, vt_ref, wt_ref, a_ref):
    core = core_ref[0]
    rows, width = vec_ref.shape
    sublane = lax.broadcasted_iota(jnp.int32, (8, 256), 0)
    for block in range(width // LANES):
        for g in range(rows // LANES):
            vt_ref[block * LANES : (block + 1) * LANES, g * LANES : (g + 1) * LANES] = vec_ref[
                g * LANES : (g + 1) * LANES, block * LANES : (block + 1) * LANES
            ].T

    def some_subspaces(step, carry):
        codes = codes_ref[pl.ds(pl.multiple_of(step * 8, 8), 8), :]
        stack = []
        for i in range(8):
            m = step * 8 + i
            shard, within = m // 6, m % 6
            half, j = within // 3, within % 3
            base = shard * 8 + j * 2
            mine = half == core
            words = []
            for h in range(2):
                spot = pl.ds(base + h, 8, stride=LANES)
                words.append(jnp.where(mine, own_ref[spot, :], sib_ref[spot, :]))
            at = pl.ds(pl.multiple_of(m * 8, 8), 8)
            for g in range(rows // LANES):
                cut = slice(g * LANES, (g + 1) * LANES)
                code = jnp.broadcast_to(codes[i : i + 1, cut], (8, LANES))
                low = code & (LANES - 1)
                first = jnp.take_along_axis(words[0], low, axis=1, mode="promise_in_bounds")
                second = jnp.take_along_axis(words[1], low, axis=1, mode="promise_in_bounds")
                wt_ref[at, cut] = vt_ref[at, cut] - jnp.where(code >= LANES, second, first)
            both = jnp.concatenate(words, axis=1)
            norm = jnp.sum(both * both, axis=0, keepdims=True)
            hi, mid, lo = three_way(-2.0 * both)
            nhi, nmid, nlo = three_way(norm)
            norms = jnp.where(sublane == 0, nhi, jnp.where(sublane == 1, nmid, jnp.where(sublane == 2, nlo, 0.0)))
            stack += [hi, hi, hi, mid, mid, lo, norms, jnp.zeros_like(norms)]
            if i % 2 == 1:
                a_ref[m // 2] = jnp.concatenate(stack, axis=0).T.astype(jnp.bfloat16)
                stack = []
        return carry

    lax.fori_loop(0, codes_ref.shape[0] // 8, some_subspaces, 0)


PARTS = 8


def pick_kernel(start_ref, cent_ref, out_hbm, out_ref, sems):
    tiles = 6
    words = out_ref.shape[0] // PARTS
    slots = words // tiles
    copies = []
    for part in range(PARTS):

        def some(i, carry, part=part):
            for k in range(32):
                row = cent_ref[pl.ds(start_ref[part * slots + i * 32 + k], tiles, stride=8), :]
                out_ref[pl.ds(part * words + (i * 4 + k // 8) * (8 * tiles) + k % 8, tiles, stride=8), :] = row
            return carry

        lax.fori_loop(0, slots // 32, some, 0)
        cut = slice(part * words, (part + 1) * words)
        copies.append(pltpu.make_async_copy(out_ref.at[cut], out_hbm.at[cut], sems.at[part]))
        copies[-1].start()
    for copy in copies:
        copy.wait()


def tiled_view(x):
    n, w = x.shape
    return x.reshape(n // 8, 8, w // LANES, LANES).swapaxes(1, 2).reshape(n * w // LANES, LANES)


def untiled_view(x, n, w):
    return x.reshape(n // 8, w // LANES, 8, LANES).swapaxes(1, 2).reshape(n, w)


STAGES = ((0, 1), (1, 3), (3, 6))


def score_kernel(vt_hbm, wt_hbm, cent_ref, a_hbm, live_ref, coded_ref, best_ref, vt_ref, wt_ref, a_ref, acc_ref, sems):
    rows, width = cent_ref.shape
    wide = 256

    def fetch(k):
        lo, hi = STAGES[k]
        pairs, feats = slice(lo * 8, hi * 8), slice(lo * LANES, hi * LANES)
        copies = [
            pltpu.make_async_copy(a_hbm.at[pairs], a_ref.at[pairs], sems.at[k, 0]),
            pltpu.make_async_copy(vt_hbm.at[feats], vt_ref.at[feats], sems.at[k, 1]),
        ]
        if k > 0:
            feats = slice(0 if k == 1 else lo * LANES, hi * LANES)
            copies.append(pltpu.make_async_copy(wt_hbm.at[feats], wt_ref.at[feats], sems.at[k, 2]))
        for copy in copies:
            copy.start()
        return copies

    def turned(block, t):
        spots = [slice(t * wide + g * LANES, t * wide + (g + 1) * LANES) for g in range(wide // LANES)]
        return jnp.concatenate([cent_ref[at, block * LANES : (block + 1) * LANES].T for at in spots], axis=1)

    waiting = [fetch(0)]
    acc_ref[...] = jnp.zeros_like(acc_ref)
    ones = jnp.ones((16, wide), jnp.bfloat16)
    none = jnp.zeros((SPLITS, wide), jnp.bfloat16)
    for k, (lo, hi) in enumerate(STAGES):
        for copy in waiting[k]:
            copy.wait()
        if k == 0:
            waiting += [fetch(j) for j in range(1, len(STAGES))]
        for block in range(lo, hi):
            feats = slice(block * LANES, (block + 1) * LANES)
            for t in range(rows // wide):
                cut = slice(t * wide, (t + 1) * wide)
                cent = turned(block, t)
                resid = vt_ref[feats, cut] - cent
                least = jnp.zeros((1, wide), jnp.float32)
                for pair in range(8):
                    left = a_ref[block * 8 + pair]
                    for half in range(2):
                        at = (pair * 2 + half) * 8
                        top, mid, low = three_way(resid[at : at + 8, :])
                        side = [
                            jnp.concatenate([top, mid], axis=0).astype(jnp.bfloat16),
                            jnp.concatenate([low, top], axis=0).astype(jnp.bfloat16),
                            jnp.concatenate([mid, top], axis=0).astype(jnp.bfloat16),
                            ones,
                        ]
                        side = [none] + side if half else side + [none]
                        table = jnp.dot(left, jnp.concatenate(side, axis=0), preferred_element_type=jnp.float32)
                        least += jnp.min(table, axis=0, keepdims=True)
                acc_ref[8:16, cut] += jnp.sum((resid * resid).reshape(16, 8, wide), axis=0)
                acc_ref[16:17, cut] += least
                if k > 0:
                    err = wt_ref[feats, cut] - cent
                    acc_ref[0:8, cut] += jnp.sum((err * err).reshape(16, 8, wide), axis=0)
                if block == 1:
                    err = wt_ref[0:LANES, cut] - turned(0, t)
                    acc_ref[0:8, cut] += jnp.sum((err * err).reshape(16, 8, wide), axis=0)
    live = live_ref[...] != 0
    coded = jnp.sum(acc_ref[0:8, :], axis=0, keepdims=True)
    best = jnp.sum(acc_ref[8:16, :], axis=0, keepdims=True) + acc_ref[16:17, :]
    coded_ref[...] = jnp.where(live, coded, 0.0)
    best_ref[...] = jnp.where(live, best, 0.0)


def pack_kernel(ids_hbm, book_hbm, lists_hbm, out_hbm, lists_ref, ids_ref, book_ref, out_ref, sems):
    fetches = [
        pltpu.make_async_copy(book_hbm, book_ref, sems.at[0]),
        pltpu.make_async_copy(ids_hbm, ids_ref, sems.at[1]),
        pltpu.make_async_copy(lists_hbm, lists_ref, sems.at[2]),
    ]
    for fetch in fetches:
        fetch.start()
    u = lax.axis_index("row")
    rows = ids_ref.shape[0]
    cols = out_ref.shape[0] // rows
    fetches[0].wait()
    fetches[1].wait()
    mine = book_ref[pl.ds(u, 12, stride=8), :]
    for r in range(rows):
        half = mine[(r % 2) * 6 : (r % 2) * 6 + 6, :]
        ids = ids_ref[r : r + 1, :].astype(jnp.float32)
        tile = jnp.concatenate([half, ids, ids], axis=0)
        out_ref[r * cols : (r + 1) * cols] = jnp.broadcast_to(tile[None], (cols, 8, LANES))
    send = pltpu.make_async_copy(out_ref, out_hbm, sems.at[3])
    send.start()
    fetches[2].wait()
    send.wait()


def pinned(x):
    return pltpu.with_memory_space_constraint(x, pltpu.HBM)


def local(vectors, list_ids, pq_codes, fill_counts, centroids, codebook):
    row_count = lax.axis_size("row")
    col_count = lax.axis_size("col")
    devices = row_count * col_count
    slots, width = vectors.shape
    cap = slots // devices
    subs = pq_codes.shape[1]
    f32 = jnp.float32
    my_row = lax.axis_index("row")
    core = my_row % 2

    per_row = LANES // cap
    vmem = pl.BlockSpec(memory_space=pltpu.VMEM)
    smem = pl.BlockSpec(memory_space=pltpu.SMEM)
    hbm = pl.BlockSpec(memory_space=pltpu.HBM)
    sent, lists = pl.pallas_call(
        pack_kernel,
        in_specs=[hbm, hbm, hbm],
        out_specs=[hbm, vmem],
        out_shape=[
            pltpu.HBM((devices, 8, LANES), f32),
            pltpu.VMEM((centroids.size // LANES, LANES), f32),
        ],
        scratch_shapes=[
            pltpu.VMEM((row_count, LANES), jnp.int32),
            pltpu.VMEM((codebook.size // LANES, LANES), f32),
            pltpu.VMEM((devices, 8, LANES), f32),
            pltpu.SemaphoreType.DMA((4,)),
        ],
        compiler_params=pltpu.CompilerParams(vmem_limit_bytes=4 << 20),
        name="pack",
    )(
        pinned(list_ids.reshape(row_count, LANES)),
        pinned(tiled_view(codebook.reshape(-1, codebook.shape[2]))),
        pinned(tiled_view(centroids)),
    )
    got = lax.all_to_all(sent, BOTH, 0, 0, tiled=True)
    sibling = lax.ppermute(got, "row", [(i, i ^ 1) for i in range(row_count)])

    me = my_row * col_count + lax.axis_index("col")
    want = lax.dynamic_slice(got[:, 6], (0, (me % per_row) * cap), (devices, cap))
    want = want.astype(jnp.int32).reshape(slots) % centroids.shape[0]
    start = (want // 8) * (8 * width // LANES) + want % 8
    picked = pl.pallas_call(
        pick_kernel,
        in_specs=[smem, vmem],
        out_specs=hbm,
        out_shape=pltpu.HBM((slots * width // LANES, LANES), f32),
        scratch_shapes=[pltpu.VMEM((slots * width // LANES, LANES), f32), pltpu.SemaphoreType.DMA((PARTS,))],
        compiler_params=pltpu.CompilerParams(vmem_limit_bytes=8 << 20),
        name="pick",
    )(start, lists)
    picked = untiled_view(picked, slots, width)
    cent = lax.all_to_all(picked.reshape(devices, cap, width), BOTH, 0, 0, tiled=True)
    cent = cent.reshape(slots, width)

    vt, wt, a = pl.pallas_call(
        prep_kernel,
        in_specs=[smem, vmem, vmem, vmem, vmem],
        out_specs=[vmem] * 3,
        out_shape=[
            jax.ShapeDtypeStruct((width, slots), f32),
            jax.ShapeDtypeStruct((width, slots), f32),
            jax.ShapeDtypeStruct((subs // 2, 256, LANES), jnp.bfloat16),
        ],
        compiler_params=pltpu.CompilerParams(vmem_limit_bytes=24 << 20),
        name="prep",
    )(
        core.reshape(1).astype(jnp.int32),
        vectors,
        pq_codes.T,
        got.reshape(devices * 8, LANES),
        sibling.reshape(devices * 8, LANES),
    )

    slot_pos = jnp.arange(cap, dtype=jnp.int32)
    live = (slot_pos[None, :] < fill_counts[0][:, None]).astype(jnp.int32).reshape(1, slots)
    coded, best = pl.pallas_call(
        score_kernel,
        in_specs=[hbm, hbm, vmem, hbm, vmem],
        out_specs=[vmem] * 2,
        out_shape=[jax.ShapeDtypeStruct((1, slots), f32)] * 2,
        scratch_shapes=[
            pltpu.VMEM((width, slots), f32),
            pltpu.VMEM((width, slots), f32),
            pltpu.VMEM((subs // 2, 256, LANES), jnp.bfloat16),
            pltpu.VMEM((24, slots), f32),
            pltpu.SemaphoreType.DMA((len(STAGES), 3)),
        ],
        compiler_params=pltpu.CompilerParams(vmem_limit_bytes=32 << 20),
        name="score",
    )(pinned(vt), pinned(wt), cent, pinned(a), live)
    return coded.reshape(slots), best.reshape(slots)


def solution(mesh):
    in_specs = (
        P(BOTH, None),
        P(BOTH),
        P(BOTH, None),
        P(BOTH, None),
        P(BOTH, None),
        P("col", None, None),
    )
    out_specs = (P(BOTH), P(BOTH))
    return jax.shard_map(local, mesh=mesh, in_specs=in_specs, out_specs=out_specs, check_vma=False)
```

```python
import jax
import jax.numpy as jnp
from jax import lax
from jax.experimental import pallas as pl
from jax.experimental.pallas import tpu as pltpu
from jax.sharding import PartitionSpec as P

BOTH = ("row", "col")
LANES = 128
SPLITS = 64


def three_way(x):
    hi = x.astype(jnp.bfloat16).astype(jnp.float32)
    rest = x - hi
    mid = rest.astype(jnp.bfloat16).astype(jnp.float32)
    lo = (rest - mid).astype(jnp.bfloat16).astype(jnp.float32)
    return hi, mid, lo


KEPT = 4


def head_rows(ref, first, block):
    tiles = 6
    top = lax.broadcasted_iota(jnp.int32, (8, LANES), 0) < KEPT
    rows = []
    for e in range(16):
        at = (first + 2 * e) * 8 * tiles + block * 8
        even, odd = ref[at : at + 8, :], ref[at + 8 * tiles : at + 8 * tiles + 8, :]
        rows.append(jnp.where(top, even, pltpu.roll(odd, KEPT, axis=0)))
    return jnp.concatenate(rows, axis=0)


def tail_rows(ref, first, block):
    tiles = 6
    spots = [(first // 8 + e) * 8 * tiles + block * 8 for e in range(16)]
    return jnp.concatenate([ref[at : at + 8, :] for at in spots], axis=0)


def prep_kernel(
    core_ref, fill_ref, vec_ref, codes_ref, own_ref, sib_ref, vt_hbm, w_hbm, a_hbm, list_ref, vt_ref, w_ref, a_ref, tail_ref, sems
):
    core = core_ref[0]
    tiles = 6
    pairs = fill_ref.shape[0]
    rows = pairs * 8
    tail = rows // 2
    sublane = lax.broadcasted_iota(jnp.int32, (8, 256), 0)

    def no_row(i, carry):
        list_ref[i] = 0
        return carry

    def one_pair(d, at):
        for j in range(KEPT, 8):
            list_ref[at + j - KEPT] = d * (8 * tiles) + j
        return at + jnp.maximum(fill_ref[d] - KEPT, 0)

    lax.fori_loop(0, list_ref.shape[0], no_row, 0)
    lax.fori_loop(0, pairs, one_pair, 0)

    def some(i, carry):
        for k in range(32):
            row = vec_ref[pl.ds(list_ref[i * 32 + k], tiles, stride=8), :]
            tail_ref[pl.ds((i * 4 + k // 8) * (8 * tiles) + k % 8, tiles, stride=8), :] = row
        return carry

    lax.fori_loop(0, tail // 32, some, 0)
    for block in range(tiles):
        feats = slice(block * LANES, (block + 1) * LANES)
        for g in range(tail // LANES):
            vt_ref[feats, g * LANES : (g + 1) * LANES] = head_rows(vec_ref, g * 32, block).T
            vt_ref[feats, tail + g * LANES : tail + (g + 1) * LANES] = tail_rows(tail_ref, g * LANES, block).T
    sent = [pltpu.make_async_copy(vt_ref, vt_hbm, sems.at[0])]
    sent[0].start()

    def one_block(block, carry):
        codes = codes_ref[pl.ds(pl.multiple_of(block * 16, 16), 16), :]
        stack = []
        words_of = []
        for i in range(16):
            m = block * 16 + i
            shard, within = m // 6, m % 6
            half, j = within // 3, within % 3
            base = shard * 8 + j * 2
            mine = half == core
            words = []
            for h in range(2):
                spot = pl.ds(base + h, 8, stride=LANES)
                words.append(jnp.where(mine, own_ref[spot, :], sib_ref[spot, :]))
            words_of.append(words)
            both = jnp.concatenate(words, axis=1)
            norm = jnp.sum(both * both, axis=0, keepdims=True)
            hi, mid, lo = three_way(-2.0 * both)
            nhi, nmid, nlo = three_way(norm)
            norms = jnp.where(sublane == 0, nhi, jnp.where(sublane == 1, nmid, jnp.where(sublane == 2, nlo, 0.0)))
            stack += [hi, hi, hi, mid, mid, lo, norms, jnp.zeros_like(norms)]
            if i % 2 == 1:
                a_ref[m // 2] = jnp.concatenate(stack, axis=0).T.astype(jnp.bfloat16)
                stack = []
        for g in range(rows // LANES):
            cut = slice(g * LANES, (g + 1) * LANES)
            coded = []
            for i in range(16):
                code = jnp.broadcast_to(codes[i : i + 1, cut], (8, LANES))
                low = code & (LANES - 1)
                first = jnp.take_along_axis(words_of[i][0], low, axis=1, mode="promise_in_bounds")
                second = jnp.take_along_axis(words_of[i][1], low, axis=1, mode="promise_in_bounds")
                coded.append(jnp.where(code >= LANES, second, first))
            turned = jnp.concatenate(coded, axis=0).T
            for e in range(16):
                at = pl.ds(pl.multiple_of((g * 16 + e) * (8 * tiles) + block * 8, 8), 8)
                w_ref[at, :] = vec_ref[at, :] - turned[e * 8 : (e + 1) * 8, :]
        return carry

    lax.fori_loop(0, tiles, one_block, 0)
    sent += [
        pltpu.make_async_copy(w_ref, w_hbm, sems.at[1]),
        pltpu.make_async_copy(a_ref, a_hbm, sems.at[2]),
    ]
    for copy in sent[1:]:
        copy.start()
    for copy in sent:
        copy.wait()


PARTS = 8


def pick_kernel(start_ref, cent_ref, out_hbm, out_ref, sems):
    tiles = 6
    words = out_ref.shape[0] // PARTS
    slots = words // tiles
    copies = []
    for part in range(PARTS):

        def some(i, carry, part=part):
            for k in range(32):
                row = cent_ref[pl.ds(start_ref[part * slots + i * 32 + k], tiles, stride=8), :]
                out_ref[pl.ds(part * words + (i * 4 + k // 8) * (8 * tiles) + k % 8, tiles, stride=8), :] = row
            return carry

        lax.fori_loop(0, slots // 32, some, 0)
        cut = slice(part * words, (part + 1) * words)
        copies.append(pltpu.make_async_copy(out_ref.at[cut], out_hbm.at[cut], sems.at[part]))
        copies[-1].start()
    for copy in copies:
        copy.wait()


def tiled_view(x):
    n, w = x.shape
    return x.reshape(n // 8, 8, w // LANES, LANES).swapaxes(1, 2).reshape(n * w // LANES, LANES)


def untiled_view(x, n, w):
    return x.reshape(n // 8, w // LANES, 8, LANES).swapaxes(1, 2).reshape(n, w)


STAGES = ((0, 1), (1, 3), (3, 6))


def score_kernel(
    list_ref, count_ref, vt_hbm, w_hbm, cent_ref, a_hbm, pos_ref, live_ref, coded_ref, best_ref, vt_ref, w_ref, a_ref, tail_ref, acc_ref, part_ref, sems
):
    tiles = 6
    rows = pos_ref.shape[0] * LANES
    wide = 256
    head = rows // 2

    def fetch(k):
        lo, hi = STAGES[k]
        pairs, feats = slice(lo * 8, hi * 8), slice(lo * LANES, hi * LANES)
        copies = [
            pltpu.make_async_copy(a_hbm.at[pairs], a_ref.at[pairs], sems.at[k, 0]),
            pltpu.make_async_copy(vt_hbm.at[feats], vt_ref.at[feats], sems.at[k, 1]),
        ]
        if hi == tiles:
            copies.append(pltpu.make_async_copy(w_hbm, w_ref, sems.at[k, 2]))
        for copy in copies:
            copy.start()
        return copies

    def gather(first):
        for k in range(wide):
            row = cent_ref[pl.ds(list_ref[first + k], tiles, stride=8), :]
            tail_ref[pl.ds(k // 8 * (8 * tiles) + k % 8, tiles, stride=8), :] = row

    ones = jnp.ones((16, wide), jnp.bfloat16)
    none = jnp.zeros((SPLITS, wide), jnp.bfloat16)

    def score(block, t):
        cut = slice(t * wide, (t + 1) * wide)
        if t * wide < head:
            cent = [head_rows(cent_ref, t * 64 + g * 32, block).T for g in range(2)]
        else:
            cent = [tail_rows(tail_ref, g * LANES, block).T for g in range(2)]
        resid = vt_ref[block * LANES : (block + 1) * LANES, cut] - jnp.concatenate(cent, axis=1)
        least = jnp.zeros((1, wide), jnp.float32)
        for pair in range(8):
            left = a_ref[block * 8 + pair]
            for half in range(2):
                at = (pair * 2 + half) * 8
                top, mid, low = three_way(resid[at : at + 8, :])
                side = [
                    jnp.concatenate([top, mid], axis=0).astype(jnp.bfloat16),
                    jnp.concatenate([low, top], axis=0).astype(jnp.bfloat16),
                    jnp.concatenate([mid, top], axis=0).astype(jnp.bfloat16),
                    ones,
                ]
                side = [none] + side if half else side + [none]
                table = jnp.dot(left, jnp.concatenate(side, axis=0), preferred_element_type=jnp.float32)
                least += jnp.min(table, axis=0, keepdims=True)
        acc_ref[0:8, cut] += jnp.sum((resid * resid).reshape(16, 8, wide), axis=0)
        acc_ref[8:9, cut] += least

    waiting = [fetch(0)]
    acc_ref[...] = jnp.zeros_like(acc_ref)
    gather(0)
    for k, (lo, hi) in enumerate(STAGES):
        for copy in waiting[k]:
            copy.wait()
        if k == 0:
            waiting += [fetch(1), fetch(2)]
        for block in range(lo, hi):
            for t in range(3):
                score(block, t)
            if hi == tiles:
                share = rows // 8 // (hi - lo) + 1
                for d in range((block - lo) * share, min((block - lo + 1) * share, rows // 8)):
                    total = jnp.zeros((8, LANES), jnp.float32)
                    for b in range(tiles):
                        at = slice((d * tiles + b) * 8, (d * tiles + b + 1) * 8)
                        err = w_ref[at, :] - cent_ref[at, :]
                        total += err * err
                    part_ref[d * 8 : (d + 1) * 8, :] = total

    @pl.when(count_ref[0] > wide)
    def _():
        gather(wide)
        for block in range(tiles):
            score(block, 3)

    best = jnp.sum(acc_ref[0:8, :], axis=0, keepdims=True) + acc_ref[8:9, :]
    pos = pos_ref[...]
    live = live_ref[...] != 0
    found = jnp.zeros(pos.shape, jnp.float32)
    for h in range(rows // LANES):
        source = jnp.broadcast_to(best[:, h * LANES : (h + 1) * LANES], pos.shape)
        lane = jnp.take_along_axis(source, pos & (LANES - 1), axis=1, mode="promise_in_bounds")
        found = jnp.where(pos // LANES == h, lane, found)
    coded = [
        jnp.sum(part_ref[h * LANES : (h + 1) * LANES, :].T, axis=0, keepdims=True) for h in range(rows // LANES)
    ]
    coded_ref[...] = jnp.where(live, jnp.concatenate(coded, axis=0), 0.0)
    best_ref[...] = jnp.where(live, found, 0.0)


def pack_kernel(ids_hbm, book_hbm, lists_hbm, out_hbm, lists_ref, ids_ref, book_ref, out_ref, sems):
    fetches = [
        pltpu.make_async_copy(book_hbm, book_ref, sems.at[0]),
        pltpu.make_async_copy(ids_hbm, ids_ref, sems.at[1]),
        pltpu.make_async_copy(lists_hbm, lists_ref, sems.at[2]),
    ]
    for fetch in fetches:
        fetch.start()
    u = lax.axis_index("row")
    rows = ids_ref.shape[0]
    cols = out_ref.shape[0] // rows
    fetches[0].wait()
    fetches[1].wait()
    mine = book_ref[pl.ds(u, 12, stride=8), :]
    for r in range(rows):
        half = mine[(r % 2) * 6 : (r % 2) * 6 + 6, :]
        ids = ids_ref[r : r + 1, :].astype(jnp.float32)
        tile = jnp.concatenate([half, ids, ids], axis=0)
        out_ref[r * cols : (r + 1) * cols] = jnp.broadcast_to(tile[None], (cols, 8, LANES))
    send = pltpu.make_async_copy(out_ref, out_hbm, sems.at[3])
    send.start()
    fetches[2].wait()
    send.wait()


def pinned(x):
    return pltpu.with_memory_space_constraint(x, pltpu.HBM)


def local(vectors, list_ids, pq_codes, fill_counts, centroids, codebook):
    row_count = lax.axis_size("row")
    col_count = lax.axis_size("col")
    devices = row_count * col_count
    slots, width = vectors.shape
    cap = slots // devices
    subs = pq_codes.shape[1]
    f32 = jnp.float32
    my_row = lax.axis_index("row")
    core = my_row % 2

    per_row = LANES // cap
    vmem = pl.BlockSpec(memory_space=pltpu.VMEM)
    smem = pl.BlockSpec(memory_space=pltpu.SMEM)
    hbm = pl.BlockSpec(memory_space=pltpu.HBM)
    sent, lists = pl.pallas_call(
        pack_kernel,
        in_specs=[hbm, hbm, hbm],
        out_specs=[hbm, vmem],
        out_shape=[
            pltpu.HBM((devices, 8, LANES), f32),
            pltpu.VMEM((centroids.size // LANES, LANES), f32),
        ],
        scratch_shapes=[
            pltpu.VMEM((row_count, LANES), jnp.int32),
            pltpu.VMEM((codebook.size // LANES, LANES), f32),
            pltpu.VMEM((devices, 8, LANES), f32),
            pltpu.SemaphoreType.DMA((4,)),
        ],
        compiler_params=pltpu.CompilerParams(vmem_limit_bytes=4 << 20),
        name="pack",
    )(
        pinned(list_ids.reshape(row_count, LANES)),
        pinned(tiled_view(codebook.reshape(-1, codebook.shape[2]))),
        pinned(tiled_view(centroids)),
    )
    got = lax.all_to_all(sent, BOTH, 0, 0, tiled=True)
    sibling = lax.ppermute(got, "row", [(i, i ^ 1) for i in range(row_count)])

    me = my_row * col_count + lax.axis_index("col")
    want = lax.dynamic_slice(got[:, 6], (0, (me % per_row) * cap), (devices, cap))
    want = want.astype(jnp.int32).reshape(slots) % centroids.shape[0]
    start = (want // 8) * (8 * width // LANES) + want % 8
    picked = pl.pallas_call(
        pick_kernel,
        in_specs=[smem, vmem],
        out_specs=hbm,
        out_shape=pltpu.HBM((slots * width // LANES, LANES), f32),
        scratch_shapes=[pltpu.VMEM((slots * width // LANES, LANES), f32), pltpu.SemaphoreType.DMA((PARTS,))],
        compiler_params=pltpu.CompilerParams(vmem_limit_bytes=8 << 20),
        name="pick",
    )(start, lists)
    picked = untiled_view(picked, slots, width)
    cent = lax.all_to_all(picked.reshape(devices, cap, width), BOTH, 0, 0, tiled=True)
    cent = tiled_view(cent.reshape(slots, width))

    fill = fill_counts[0]
    extra = jnp.maximum(fill - KEPT, 0)
    pair = jnp.arange(devices, dtype=jnp.int32)
    before = jnp.sum(jnp.where(pair[None, :] < pair[:, None], extra[None, :], 0), axis=1)
    slot = jnp.arange(cap, dtype=jnp.int32)[None, :]
    pos = jnp.where(slot < KEPT, KEPT * pair[:, None] + slot, slots // 2 + before[:, None] + slot - KEPT)
    pos = pos.reshape(slots // LANES, LANES)
    live = (slot < fill[:, None]).astype(jnp.int32).reshape(slots // LANES, LANES)

    view = (slots * width // LANES, LANES)
    book = (subs // 2, 256, LANES)
    vt, w, a, rows = pl.pallas_call(
        prep_kernel,
        in_specs=[smem, smem, vmem, vmem, vmem, vmem],
        out_specs=[hbm] * 3 + [smem],
        out_shape=[
            pltpu.HBM((width, slots), f32),
            pltpu.HBM(view, f32),
            pltpu.HBM(book, jnp.bfloat16),
            jax.ShapeDtypeStruct((slots // 2 + 8,), jnp.int32),
        ],
        scratch_shapes=[
            pltpu.VMEM((width, slots), f32),
            pltpu.VMEM(view, f32),
            pltpu.VMEM(book, jnp.bfloat16),
            pltpu.VMEM((view[0] // 2, LANES), f32),
            pltpu.SemaphoreType.DMA((3,)),
        ],
        compiler_params=pltpu.CompilerParams(vmem_limit_bytes=32 << 20),
        name="prep",
    )(
        core.reshape(1).astype(jnp.int32),
        fill,
        tiled_view(vectors),
        pq_codes.T,
        got.reshape(devices * 8, LANES),
        sibling.reshape(devices * 8, LANES),
    )

    coded, best = pl.pallas_call(
        score_kernel,
        in_specs=[smem, smem, hbm, hbm, vmem, hbm, vmem, vmem],
        out_specs=[vmem] * 2,
        out_shape=[jax.ShapeDtypeStruct((slots // LANES, LANES), f32)] * 2,
        scratch_shapes=[
            pltpu.VMEM((width, slots), f32),
            pltpu.VMEM(view, f32),
            pltpu.VMEM(book, jnp.bfloat16),
            pltpu.VMEM((view[0] // 4, LANES), f32),
            pltpu.VMEM((16, slots), f32),
            pltpu.VMEM((slots, LANES), f32),
            pltpu.SemaphoreType.DMA((len(STAGES), 3)),
        ],
        compiler_params=pltpu.CompilerParams(vmem_limit_bytes=32 << 20),
        name="score",
    )(rows, jnp.sum(extra).reshape(1), pinned(vt), pinned(w), cent, pinned(a), pos, live)
    return coded.reshape(slots), best.reshape(slots)


def solution(mesh):
    in_specs = (
        P(BOTH, None),
        P(BOTH),
        P(BOTH, None),
        P(BOTH, None),
        P(BOTH, None),
        P("col", None, None),
    )
    out_specs = (P(BOTH), P(BOTH))
    return jax.shard_map(local, mesh=mesh, in_specs=in_specs, out_specs=out_specs, check_vma=False)
```

```python
import jax
import jax.numpy as jnp
from jax import lax
from jax.experimental import pallas as pl
from jax.experimental.pallas import tpu as pltpu
from jax.sharding import PartitionSpec as P

BOTH = ("row", "col")
LANES = 128
SPLITS = 64


def three_way(x):
    hi = x.astype(jnp.bfloat16).astype(jnp.float32)
    rest = x - hi
    mid = rest.astype(jnp.bfloat16).astype(jnp.float32)
    lo = (rest - mid).astype(jnp.bfloat16).astype(jnp.float32)
    return hi, mid, lo


KEPT = 4


def head_rows(ref, first, block):
    tiles = 6
    top = lax.broadcasted_iota(jnp.int32, (8, LANES), 0) < KEPT
    rows = []
    for e in range(16):
        at = (first + 2 * e) * 8 * tiles + block * 8
        even, odd = ref[at : at + 8, :], ref[at + 8 * tiles : at + 8 * tiles + 8, :]
        rows.append(jnp.where(top, even, pltpu.roll(odd, KEPT, axis=0)))
    return jnp.concatenate(rows, axis=0)


def tail_rows(ref, first, block):
    tiles = 6
    spots = [(first // 8 + e) * 8 * tiles + block * 8 for e in range(16)]
    return jnp.concatenate([ref[at : at + 8, :] for at in spots], axis=0)


def prep_kernel(
    core_ref, fill_ref, fills_ref, vec_ref, codes_ref, own_ref, sib_ref, vt_hbm, w_hbm, a_hbm, list_hbm, pos_ref, live_ref,
    list_ref, vt_ref, w_ref, a_ref, tail_ref, sems
):
    core = core_ref[0]
    tiles = 6
    pairs = fill_ref.shape[0]
    rows = pairs * 8
    tail = rows // 2
    sublane = lax.broadcasted_iota(jnp.int32, (8, 256), 0)

    def no_row(i, carry):
        list_ref[i] = 0
        return carry

    def one_pair(d, at):
        for j in range(KEPT, 8):
            list_ref[at + j - KEPT] = d * (8 * tiles) + j
        return at + jnp.maximum(fill_ref[d] - KEPT, 0)

    lax.fori_loop(0, tail, no_row, 0)
    list_ref[list_ref.shape[0] - 1] = lax.fori_loop(0, pairs, one_pair, 0)
    sent = [pltpu.make_async_copy(list_ref, list_hbm, sems.at[3])]
    sent[0].start()

    across = lax.broadcasted_iota(jnp.int32, (pairs, pairs), 1)
    down = lax.broadcasted_iota(jnp.int32, (pairs, pairs), 0)
    spot = lax.broadcasted_iota(jnp.int32, pos_ref.shape, 0) * LANES + lax.broadcasted_iota(jnp.int32, pos_ref.shape, 1)
    slot = spot % 8
    fills = jnp.broadcast_to(fills_ref[...], pos_ref.shape)
    extra = jnp.maximum(fills - KEPT, 0).astype(jnp.float32).astype(jnp.bfloat16)
    earlier = jnp.where(down < across, 1.0, 0.0).astype(jnp.bfloat16)
    before = jnp.dot(extra, earlier, preferred_element_type=jnp.float32).astype(jnp.int32)
    fill_of = jnp.take_along_axis(fills, spot // 8, axis=1, mode="promise_in_bounds")
    before_of = jnp.take_along_axis(before, spot // 8, axis=1, mode="promise_in_bounds")
    pos_ref[...] = jnp.where(slot < KEPT, KEPT * (spot // 8) + slot, tail + before_of + slot - KEPT)
    live_ref[...] = (slot < fill_of).astype(jnp.int32)

    def some(i, carry):
        for k in range(32):
            row = vec_ref[pl.ds(list_ref[i * 32 + k], tiles, stride=8), :]
            tail_ref[pl.ds((i * 4 + k // 8) * (8 * tiles) + k % 8, tiles, stride=8), :] = row
        return carry

    lax.fori_loop(0, tail // 32, some, 0)
    for block in range(tiles):
        feats = slice(block * LANES, (block + 1) * LANES)
        for g in range(tail // LANES):
            vt_ref[feats, g * LANES : (g + 1) * LANES] = head_rows(vec_ref, g * 32, block).T
            vt_ref[feats, tail + g * LANES : tail + (g + 1) * LANES] = tail_rows(tail_ref, g * LANES, block).T
    sent.append(pltpu.make_async_copy(vt_ref, vt_hbm, sems.at[0]))
    sent[1].start()

    def one_block(block, carry):
        codes = codes_ref[pl.ds(pl.multiple_of(block * 16, 16), 16), :]
        stack = []
        words_of = []
        for i in range(16):
            m = block * 16 + i
            shard, within = m // 6, m % 6
            half, j = within // 3, within % 3
            base = shard * 8 + j * 2
            mine = half == core
            words = []
            for h in range(2):
                spot = pl.ds(base + h, 8, stride=LANES)
                words.append(jnp.where(mine, own_ref[spot, :], sib_ref[spot, :]))
            words_of.append(words)
            both = jnp.concatenate(words, axis=1)
            norm = jnp.sum(both * both, axis=0, keepdims=True)
            hi, mid, lo = three_way(-2.0 * both)
            nhi, nmid, nlo = three_way(norm)
            norms = jnp.where(sublane == 0, nhi, jnp.where(sublane == 1, nmid, jnp.where(sublane == 2, nlo, 0.0)))
            stack += [hi, hi, hi, mid, mid, lo, norms, jnp.zeros_like(norms)]
            if i % 2 == 1:
                a_ref[m // 2] = jnp.concatenate(stack, axis=0).T.astype(jnp.bfloat16)
                stack = []
        for g in range(rows // LANES):
            cut = slice(g * LANES, (g + 1) * LANES)
            coded = []
            for i in range(16):
                code = jnp.broadcast_to(codes[i : i + 1, cut], (8, LANES))
                low = code & (LANES - 1)
                first = jnp.take_along_axis(words_of[i][0], low, axis=1, mode="promise_in_bounds")
                second = jnp.take_along_axis(words_of[i][1], low, axis=1, mode="promise_in_bounds")
                coded.append(jnp.where(code >= LANES, second, first))
            turned = jnp.concatenate(coded, axis=0).T
            for e in range(16):
                at = pl.ds(pl.multiple_of((g * 16 + e) * (8 * tiles) + block * 8, 8), 8)
                w_ref[at, :] = vec_ref[at, :] - turned[e * 8 : (e + 1) * 8, :]
        return carry

    lax.fori_loop(0, tiles, one_block, 0)
    sent += [
        pltpu.make_async_copy(w_ref, w_hbm, sems.at[1]),
        pltpu.make_async_copy(a_ref, a_hbm, sems.at[2]),
    ]
    for copy in sent[2:]:
        copy.start()
    for copy in sent:
        copy.wait()


PARTS = 8


def pick_kernel(start_ref, cent_ref, out_hbm, out_ref, sems):
    tiles = 6
    words = out_ref.shape[0] // PARTS
    slots = words // tiles
    copies = []
    for part in range(PARTS):

        def some(i, carry, part=part):
            for k in range(32):
                row = cent_ref[pl.ds(start_ref[part * slots + i * 32 + k], tiles, stride=8), :]
                out_ref[pl.ds(part * words + (i * 4 + k // 8) * (8 * tiles) + k % 8, tiles, stride=8), :] = row
            return carry

        lax.fori_loop(0, slots // 32, some, 0)
        cut = slice(part * words, (part + 1) * words)
        copies.append(pltpu.make_async_copy(out_ref.at[cut], out_hbm.at[cut], sems.at[part]))
        copies[-1].start()
    for copy in copies:
        copy.wait()


def tiled_view(x):
    n, w = x.shape
    return x.reshape(n // 8, 8, w // LANES, LANES).swapaxes(1, 2).reshape(n * w // LANES, LANES)


def untiled_view(x, n, w):
    return x.reshape(n // 8, w // LANES, 8, LANES).swapaxes(1, 2).reshape(n, w)


STAGES = ((0, 1), (1, 3), (3, 6))


def score_kernel(
    list_hbm, vt_hbm, w_hbm, cent_ref, a_hbm, pos_ref, live_ref, coded_ref, best_ref,
    list_ref, vt_ref, w_ref, a_ref, tail_ref, acc_ref, part_ref, sems
):
    tiles = 6
    rows = pos_ref.shape[0] * LANES
    wide = 256
    head = rows // 2
    sure = slice(0, head + wide)

    def fetch(k):
        lo, hi = STAGES[k]
        pairs, feats = slice(lo * 8, hi * 8), slice(lo * LANES, hi * LANES)
        copies = [
            pltpu.make_async_copy(a_hbm.at[pairs], a_ref.at[pairs], sems.at[k, 0]),
            pltpu.make_async_copy(vt_hbm.at[feats, sure], vt_ref.at[feats, sure], sems.at[k, 1]),
        ]
        if k == 0:
            copies.append(pltpu.make_async_copy(list_hbm, list_ref, sems.at[k, 2]))
        if hi == tiles:
            copies.append(pltpu.make_async_copy(w_hbm, w_ref, sems.at[k, 2]))
        for copy in copies:
            copy.start()
        return copies

    def gather(first):
        for k in range(wide):
            row = cent_ref[pl.ds(list_ref[first + k], tiles, stride=8), :]
            tail_ref[pl.ds(k // 8 * (8 * tiles) + k % 8, tiles, stride=8), :] = row

    ones = jnp.ones((16, wide), jnp.bfloat16)
    none = jnp.zeros((SPLITS, wide), jnp.bfloat16)

    def score(block, t):
        cut = slice(t * wide, (t + 1) * wide)
        if t * wide < head:
            cent = [head_rows(cent_ref, t * 64 + g * 32, block).T for g in range(2)]
        else:
            cent = [tail_rows(tail_ref, g * LANES, block).T for g in range(2)]
        resid = vt_ref[block * LANES : (block + 1) * LANES, cut] - jnp.concatenate(cent, axis=1)
        least = jnp.zeros((1, wide), jnp.float32)
        for pair in range(8):
            left = a_ref[block * 8 + pair]
            for half in range(2):
                at = (pair * 2 + half) * 8
                top, mid, low = three_way(resid[at : at + 8, :])
                side = [
                    jnp.concatenate([top, mid], axis=0).astype(jnp.bfloat16),
                    jnp.concatenate([low, top], axis=0).astype(jnp.bfloat16),
                    jnp.concatenate([mid, top], axis=0).astype(jnp.bfloat16),
                    ones,
                ]
                side = [none] + side if half else side + [none]
                table = jnp.dot(left, jnp.concatenate(side, axis=0), preferred_element_type=jnp.float32)
                least += jnp.min(table, axis=0, keepdims=True)
        acc_ref[0:8, cut] += jnp.sum((resid * resid).reshape(16, 8, wide), axis=0)
        acc_ref[8:9, cut] += least

    waiting = fetch(0)
    acc_ref[...] = jnp.zeros_like(acc_ref)
    for k, (lo, hi) in enumerate(STAGES):
        for copy in waiting:
            copy.wait()
        if k + 1 < len(STAGES):
            waiting = fetch(k + 1)
        for block in range(lo, hi):
            for t in range(3):
                if block == 0 and t == 2:
                    gather(0)
                score(block, t)
            if hi == tiles:
                share = rows // 8 // (hi - lo) + 1
                for d in range((block - lo) * share, min((block - lo + 1) * share, rows // 8)):
                    total = jnp.zeros((8, LANES), jnp.float32)
                    for b in range(tiles):
                        at = slice((d * tiles + b) * 8, (d * tiles + b + 1) * 8)
                        err = w_ref[at, :] - cent_ref[at, :]
                        total += err * err
                    part_ref[d * 8 : (d + 1) * 8, :] = total

    @pl.when(list_ref[list_ref.shape[0] - 1] > wide)
    def _():
        rest = slice(sure.stop, rows)
        last = pltpu.make_async_copy(vt_hbm.at[:, rest], vt_ref.at[:, rest], sems.at[0, 0])
        last.start()
        gather(wide)
        last.wait()
        for block in range(tiles):
            score(block, 3)

    best = jnp.sum(acc_ref[0:8, :], axis=0, keepdims=True) + acc_ref[8:9, :]
    pos = pos_ref[...]
    live = live_ref[...] != 0
    found = jnp.zeros(pos.shape, jnp.float32)
    for h in range(rows // LANES):
        source = jnp.broadcast_to(best[:, h * LANES : (h + 1) * LANES], pos.shape)
        lane = jnp.take_along_axis(source, pos & (LANES - 1), axis=1, mode="promise_in_bounds")
        found = jnp.where(pos // LANES == h, lane, found)
    coded = [
        jnp.sum(part_ref[h * LANES : (h + 1) * LANES, :].T, axis=0, keepdims=True) for h in range(rows // LANES)
    ]
    coded_ref[...] = jnp.where(live, jnp.concatenate(coded, axis=0), 0.0)
    best_ref[...] = jnp.where(live, found, 0.0)


def pack_kernel(ids_hbm, book_hbm, lists_hbm, out_hbm, lists_ref, ids_ref, book_ref, out_ref, sems):
    fetches = [
        pltpu.make_async_copy(book_hbm, book_ref, sems.at[0]),
        pltpu.make_async_copy(ids_hbm, ids_ref, sems.at[1]),
        pltpu.make_async_copy(lists_hbm, lists_ref, sems.at[2]),
    ]
    for fetch in fetches:
        fetch.start()
    u = lax.axis_index("row")
    rows = ids_ref.shape[0]
    cols = out_ref.shape[0] // rows
    fetches[0].wait()
    fetches[1].wait()
    mine = book_ref[pl.ds(u, 12, stride=8), :]
    for r in range(rows):
        half = mine[(r % 2) * 6 : (r % 2) * 6 + 6, :]
        ids = ids_ref[r : r + 1, :].astype(jnp.float32)
        tile = jnp.concatenate([half, ids, ids], axis=0)
        out_ref[r * cols : (r + 1) * cols] = jnp.broadcast_to(tile[None], (cols, 8, LANES))
    send = pltpu.make_async_copy(out_ref, out_hbm, sems.at[3])
    send.start()
    fetches[2].wait()
    send.wait()


def pinned(x):
    return pltpu.with_memory_space_constraint(x, pltpu.HBM)


def local(vectors, list_ids, pq_codes, fill_counts, centroids, codebook):
    row_count = lax.axis_size("row")
    col_count = lax.axis_size("col")
    devices = row_count * col_count
    slots, width = vectors.shape
    cap = slots // devices
    subs = pq_codes.shape[1]
    f32 = jnp.float32
    my_row = lax.axis_index("row")
    core = my_row % 2

    per_row = LANES // cap
    vmem = pl.BlockSpec(memory_space=pltpu.VMEM)
    smem = pl.BlockSpec(memory_space=pltpu.SMEM)
    hbm = pl.BlockSpec(memory_space=pltpu.HBM)
    sent, lists = pl.pallas_call(
        pack_kernel,
        in_specs=[hbm, hbm, hbm],
        out_specs=[hbm, vmem],
        out_shape=[
            pltpu.HBM((devices, 8, LANES), f32),
            pltpu.VMEM((centroids.size // LANES, LANES), f32),
        ],
        scratch_shapes=[
            pltpu.VMEM((row_count, LANES), jnp.int32),
            pltpu.VMEM((codebook.size // LANES, LANES), f32),
            pltpu.VMEM((devices, 8, LANES), f32),
            pltpu.SemaphoreType.DMA((4,)),
        ],
        compiler_params=pltpu.CompilerParams(vmem_limit_bytes=4 << 20),
        name="pack",
    )(
        pinned(list_ids.reshape(row_count, LANES)),
        pinned(tiled_view(codebook.reshape(-1, codebook.shape[2]))),
        pinned(tiled_view(centroids)),
    )
    got = lax.all_to_all(sent, BOTH, 0, 0, tiled=True)
    sibling = lax.ppermute(got, "row", [(i, i ^ 1) for i in range(row_count)])

    me = my_row * col_count + lax.axis_index("col")
    want = lax.dynamic_slice(got[:, 6], (0, (me % per_row) * cap), (devices, cap))
    want = want.astype(jnp.int32).reshape(slots) % centroids.shape[0]
    start = (want // 8) * (8 * width // LANES) + want % 8
    picked = pl.pallas_call(
        pick_kernel,
        in_specs=[smem, vmem],
        out_specs=hbm,
        out_shape=pltpu.HBM((slots * width // LANES, LANES), f32),
        scratch_shapes=[pltpu.VMEM((slots * width // LANES, LANES), f32), pltpu.SemaphoreType.DMA((PARTS,))],
        compiler_params=pltpu.CompilerParams(vmem_limit_bytes=8 << 20),
        name="pick",
    )(start, lists)
    picked = untiled_view(picked, slots, width)
    cent = lax.all_to_all(picked.reshape(devices, cap, width), BOTH, 0, 0, tiled=True)
    cent = tiled_view(cent.reshape(slots, width))

    view = (slots * width // LANES, LANES)
    book = (subs // 2, 256, LANES)
    vt, w, a, rows, pos, live = pl.pallas_call(
        prep_kernel,
        in_specs=[smem, smem, vmem, vmem, vmem, vmem, vmem],
        out_specs=[hbm] * 4 + [vmem] * 2,
        out_shape=[
            pltpu.HBM((width, slots), f32),
            pltpu.HBM(view, f32),
            pltpu.HBM(book, jnp.bfloat16),
            pltpu.HBM((slots,), jnp.int32),
            jax.ShapeDtypeStruct((slots // LANES, LANES), jnp.int32),
            jax.ShapeDtypeStruct((slots // LANES, LANES), jnp.int32),
        ],
        scratch_shapes=[
            pltpu.SMEM((slots,), jnp.int32),
            pltpu.VMEM((width, slots), f32),
            pltpu.VMEM(view, f32),
            pltpu.VMEM(book, jnp.bfloat16),
            pltpu.VMEM((view[0] // 2, LANES), f32),
            pltpu.SemaphoreType.DMA((4,)),
        ],
        compiler_params=pltpu.CompilerParams(vmem_limit_bytes=32 << 20),
        name="prep",
    )(
        core.reshape(1).astype(jnp.int32),
        fill_counts[0],
        fill_counts,
        tiled_view(vectors),
        pq_codes.T,
        got.reshape(devices * 8, LANES),
        sibling.reshape(devices * 8, LANES),
    )

    coded, best = pl.pallas_call(
        score_kernel,
        in_specs=[hbm, hbm, hbm, vmem, hbm, vmem, vmem],
        out_specs=[vmem] * 2,
        out_shape=[jax.ShapeDtypeStruct((slots // LANES, LANES), f32)] * 2,
        scratch_shapes=[
            pltpu.SMEM((slots,), jnp.int32),
            pltpu.VMEM((width, slots), f32),
            pltpu.VMEM(view, f32),
            pltpu.VMEM(book, jnp.bfloat16),
            pltpu.VMEM((view[0] // 4, LANES), f32),
            pltpu.VMEM((16, slots), f32),
            pltpu.VMEM((slots, LANES), f32),
            pltpu.SemaphoreType.DMA((len(STAGES), 3)),
        ],
        compiler_params=pltpu.CompilerParams(vmem_limit_bytes=32 << 20),
        name="score",
    )(pinned(rows), pinned(vt), pinned(w), cent, pinned(a), pos, live)
    return coded.reshape(slots), best.reshape(slots)


def solution(mesh):
    in_specs = (
        P(BOTH, None),
        P(BOTH),
        P(BOTH, None),
        P(BOTH, None),
        P(BOTH, None),
        P("col", None, None),
    )
    out_specs = (P(BOTH), P(BOTH))
    return jax.shard_map(local, mesh=mesh, in_specs=in_specs, out_specs=out_specs, check_vma=False)
```

```python
import jax
import jax.numpy as jnp
from jax import lax
from jax.experimental import pallas as pl
from jax.experimental.pallas import tpu as pltpu
from jax.sharding import PartitionSpec as P

BOTH = ("row", "col")
LANES = 128
SPLITS = 64


def three_way(x):
    hi = x.astype(jnp.bfloat16).astype(jnp.float32)
    rest = x - hi
    mid = rest.astype(jnp.bfloat16).astype(jnp.float32)
    lo = (rest - mid).astype(jnp.bfloat16).astype(jnp.float32)
    return hi, mid, lo


KEPT = 4


def head_rows(ref, first, block):
    tiles = 6
    top = lax.broadcasted_iota(jnp.int32, (8, LANES), 0) < KEPT
    rows = []
    for e in range(16):
        at = (first + 2 * e) * 8 * tiles + block * 8
        even, odd = ref[at : at + 8, :], ref[at + 8 * tiles : at + 8 * tiles + 8, :]
        rows.append(jnp.where(top, even, pltpu.roll(odd, KEPT, axis=0)))
    return jnp.concatenate(rows, axis=0)


def tail_rows(ref, first, block):
    tiles = 6
    spots = [(first // 8 + e) * 8 * tiles + block * 8 for e in range(16)]
    return jnp.concatenate([ref[at : at + 8, :] for at in spots], axis=0)


def prep_kernel(
    core_ref, fill_ref, fills_ref, vec_ref, codes_ref, own_ref, sib_ref, vt_hbm, w_hbm, a_hbm, list_hbm, pos_ref, live_ref,
    list_ref, vt_ref, w_ref, a_ref, tail_ref, sems
):
    core = core_ref[0]
    tiles = 6
    pairs = fill_ref.shape[0]
    rows = pairs * 8
    tail = rows // 2
    sublane = lax.broadcasted_iota(jnp.int32, (8, 256), 0)

    def no_row(i, carry):
        list_ref[i] = 0
        return carry

    def one_pair(d, at):
        for j in range(KEPT, 8):
            list_ref[at + j - KEPT] = d * (8 * tiles) + j
        return at + jnp.maximum(fill_ref[d] - KEPT, 0)

    lax.fori_loop(0, tail, no_row, 0)
    list_ref[list_ref.shape[0] - 1] = lax.fori_loop(0, pairs, one_pair, 0)
    sent = [pltpu.make_async_copy(list_ref, list_hbm, sems.at[3])]
    sent[0].start()

    across = lax.broadcasted_iota(jnp.int32, (pairs, pairs), 1)
    down = lax.broadcasted_iota(jnp.int32, (pairs, pairs), 0)
    spot = lax.broadcasted_iota(jnp.int32, pos_ref.shape, 0) * LANES + lax.broadcasted_iota(jnp.int32, pos_ref.shape, 1)
    slot = spot % 8
    fills = jnp.broadcast_to(fills_ref[...], pos_ref.shape)
    extra = jnp.maximum(fills - KEPT, 0).astype(jnp.float32).astype(jnp.bfloat16)
    earlier = jnp.where(down < across, 1.0, 0.0).astype(jnp.bfloat16)
    before = jnp.dot(extra, earlier, preferred_element_type=jnp.float32).astype(jnp.int32)
    fill_of = jnp.take_along_axis(fills, spot // 8, axis=1, mode="promise_in_bounds")
    before_of = jnp.take_along_axis(before, spot // 8, axis=1, mode="promise_in_bounds")
    pos_ref[...] = jnp.where(slot < KEPT, KEPT * (spot // 8) + slot, tail + before_of + slot - KEPT)
    live_ref[...] = (slot < fill_of).astype(jnp.int32)

    def some(i, carry):
        for k in range(32):
            row = vec_ref[pl.ds(list_ref[i * 32 + k], tiles, stride=8), :]
            tail_ref[pl.ds((i * 4 + k // 8) * (8 * tiles) + k % 8, tiles, stride=8), :] = row
        return carry

    lax.fori_loop(0, tail // 32, some, 0)
    for block in range(tiles):
        feats = slice(block * LANES, (block + 1) * LANES)
        for g in range(tail // LANES):
            vt_ref[feats, g * LANES : (g + 1) * LANES] = head_rows(vec_ref, g * 32, block).T
            vt_ref[feats, tail + g * LANES : tail + (g + 1) * LANES] = tail_rows(tail_ref, g * LANES, block).T
    sent.append(pltpu.make_async_copy(vt_ref, vt_hbm, sems.at[0]))
    sent[1].start()

    def one_block(block, carry):
        codes = codes_ref[pl.ds(pl.multiple_of(block * 16, 16), 16), :]
        stack = []
        words_of = []
        for i in range(16):
            m = block * 16 + i
            shard, within = m // 6, m % 6
            half, j = within // 3, within % 3
            base = shard * 8 + j * 2
            mine = half == core
            words = []
            for h in range(2):
                spot = pl.ds(base + h, 8, stride=LANES)
                words.append(jnp.where(mine, own_ref[spot, :], sib_ref[spot, :]))
            words_of.append(words)
            both = jnp.concatenate(words, axis=1)
            norm = jnp.sum(both * both, axis=0, keepdims=True)
            hi, mid, lo = three_way(-2.0 * both)
            nhi, nmid, nlo = three_way(norm)
            norms = jnp.where(sublane == 0, nhi, jnp.where(sublane == 1, nmid, jnp.where(sublane == 2, nlo, 0.0)))
            stack += [hi, hi, hi, mid, mid, lo, norms, jnp.zeros_like(norms)]
            if i % 2 == 1:
                a_ref[m // 2] = jnp.concatenate(stack, axis=0).T.astype(jnp.bfloat16)
                stack = []
        for g in range(rows // LANES):
            cut = slice(g * LANES, (g + 1) * LANES)
            coded = []
            for i in range(16):
                code = jnp.broadcast_to(codes[i : i + 1, cut], (8, LANES))
                low = code & (LANES - 1)
                first = jnp.take_along_axis(words_of[i][0], low, axis=1, mode="promise_in_bounds")
                second = jnp.take_along_axis(words_of[i][1], low, axis=1, mode="promise_in_bounds")
                coded.append(jnp.where(code >= LANES, second, first))
            turned = jnp.concatenate(coded, axis=0).T
            for e in range(16):
                at = pl.ds(pl.multiple_of((g * 16 + e) * (8 * tiles) + block * 8, 8), 8)
                w_ref[at, :] = vec_ref[at, :] - turned[e * 8 : (e + 1) * 8, :]
        return carry

    lax.fori_loop(0, tiles, one_block, 0)
    sent += [
        pltpu.make_async_copy(w_ref, w_hbm, sems.at[1]),
        pltpu.make_async_copy(a_ref, a_hbm, sems.at[2]),
    ]
    for copy in sent[2:]:
        copy.start()
    for copy in sent:
        copy.wait()


PARTS = 8


def pick_kernel(start_ref, cent_ref, out_hbm, out_ref, sems):
    tiles = 6
    words = out_ref.shape[0] // PARTS
    slots = words // tiles
    copies = []
    for part in range(PARTS):

        def some(i, carry, part=part):
            for k in range(32):
                row = cent_ref[pl.ds(start_ref[part * slots + i * 32 + k], tiles, stride=8), :]
                out_ref[pl.ds(part * words + (i * 4 + k // 8) * (8 * tiles) + k % 8, tiles, stride=8), :] = row
            return carry

        lax.fori_loop(0, slots // 32, some, 0)
        cut = slice(part * words, (part + 1) * words)
        copies.append(pltpu.make_async_copy(out_ref.at[cut], out_hbm.at[cut], sems.at[part]))
        copies[-1].start()
    for copy in copies:
        copy.wait()


def tiled_view(x):
    n, w = x.shape
    return x.reshape(n // 8, 8, w // LANES, LANES).swapaxes(1, 2).reshape(n * w // LANES, LANES)


def untiled_view(x, n, w):
    return x.reshape(n // 8, w // LANES, 8, LANES).swapaxes(1, 2).reshape(n, w)


STAGES = ((0, 1), (1, 3), (3, 6))


def score_kernel(
    list_hbm, vt_hbm, w_hbm, cent_ref, a_hbm, pos_ref, live_ref, coded_ref, best_ref,
    list_ref, vt_ref, w_ref, a_ref, tail_ref, acc_ref, part_ref, sems
):
    tiles = 6
    rows = pos_ref.shape[0] * LANES
    wide = 256
    head = rows // 2
    sure = slice(0, head + wide)

    def fetch(k):
        lo, hi = STAGES[k]
        pairs, feats = slice(lo * 8, hi * 8), slice(lo * LANES, hi * LANES)
        copies = [
            pltpu.make_async_copy(a_hbm.at[pairs], a_ref.at[pairs], sems.at[k, 0]),
            pltpu.make_async_copy(vt_hbm.at[feats, sure], vt_ref.at[feats, sure], sems.at[k, 1]),
        ]
        if hi == tiles:
            copies.append(pltpu.make_async_copy(w_hbm, w_ref, sems.at[k, 2]))
        for copy in copies:
            copy.start()
        return copies

    def gather(first):
        for k in range(wide):
            row = cent_ref[pl.ds(list_ref[first + k], tiles, stride=8), :]
            tail_ref[pl.ds(k // 8 * (8 * tiles) + k % 8, tiles, stride=8), :] = row

    ones = jnp.ones((16, wide), jnp.bfloat16)
    none = jnp.zeros((SPLITS, wide), jnp.bfloat16)

    def score(block, t):
        cut = slice(t * wide, (t + 1) * wide)
        if t * wide < head:
            cent = [head_rows(cent_ref, t * 64 + g * 32, block).T for g in range(2)]
        else:
            cent = [tail_rows(tail_ref, g * LANES, block).T for g in range(2)]
        resid = vt_ref[block * LANES : (block + 1) * LANES, cut] - jnp.concatenate(cent, axis=1)
        least = jnp.zeros((1, wide), jnp.float32)
        for pair in range(8):
            left = a_ref[block * 8 + pair]
            for half in range(2):
                at = (pair * 2 + half) * 8
                top, mid, low = three_way(resid[at : at + 8, :])
                side = [
                    jnp.concatenate([top, mid], axis=0).astype(jnp.bfloat16),
                    jnp.concatenate([low, top], axis=0).astype(jnp.bfloat16),
                    jnp.concatenate([mid, top], axis=0).astype(jnp.bfloat16),
                    ones,
                ]
                side = [none] + side if half else side + [none]
                table = jnp.dot(left, jnp.concatenate(side, axis=0), preferred_element_type=jnp.float32)
                least += jnp.min(table, axis=0, keepdims=True)
        acc_ref[0:8, cut] += jnp.sum((resid * resid).reshape(16, 8, wide), axis=0)
        acc_ref[8:9, cut] += least

    order = pltpu.make_async_copy(list_hbm, list_ref, sems.at[0, 2])
    order.start()
    waiting = fetch(0)
    acc_ref[...] = jnp.zeros_like(acc_ref)
    order.wait()
    gather(0)
    for k, (lo, hi) in enumerate(STAGES):
        for copy in waiting:
            copy.wait()
        if k + 1 < len(STAGES):
            waiting = fetch(k + 1)
        for block in range(lo, hi):
            for t in range(3):
                score(block, t)
            if hi == tiles:
                share = rows // 8 // (hi - lo) + 1
                for d in range((block - lo) * share, min((block - lo + 1) * share, rows // 8)):
                    total = jnp.zeros((8, LANES), jnp.float32)
                    for b in range(tiles):
                        at = slice((d * tiles + b) * 8, (d * tiles + b + 1) * 8)
                        err = w_ref[at, :] - cent_ref[at, :]
                        total += err * err
                    part_ref[d * 8 : (d + 1) * 8, :] = total

    live = live_ref[...] != 0
    coded = [
        jnp.sum(part_ref[h * LANES : (h + 1) * LANES, :].T, axis=0, keepdims=True) for h in range(rows // LANES)
    ]
    coded_ref[...] = jnp.where(live, jnp.concatenate(coded, axis=0), 0.0)

    @pl.when(list_ref[list_ref.shape[0] - 1] > wide)
    def _():
        rest = slice(sure.stop, rows)
        last = pltpu.make_async_copy(vt_hbm.at[:, rest], vt_ref.at[:, rest], sems.at[0, 0])
        last.start()
        gather(wide)
        last.wait()
        for block in range(tiles):
            score(block, 3)

    best = jnp.sum(acc_ref[0:8, :], axis=0, keepdims=True) + acc_ref[8:9, :]
    pos = pos_ref[...]
    found = jnp.zeros(pos.shape, jnp.float32)
    for h in range(rows // LANES):
        source = jnp.broadcast_to(best[:, h * LANES : (h + 1) * LANES], pos.shape)
        lane = jnp.take_along_axis(source, pos & (LANES - 1), axis=1, mode="promise_in_bounds")
        found = jnp.where(pos // LANES == h, lane, found)
    best_ref[...] = jnp.where(live_ref[...] != 0, found, 0.0)


def pack_kernel(ids_hbm, book_hbm, lists_hbm, out_hbm, lists_ref, ids_ref, book_ref, out_ref, sems):
    fetches = [
        pltpu.make_async_copy(book_hbm, book_ref, sems.at[0]),
        pltpu.make_async_copy(ids_hbm, ids_ref, sems.at[1]),
        pltpu.make_async_copy(lists_hbm, lists_ref, sems.at[2]),
    ]
    for fetch in fetches:
        fetch.start()
    u = lax.axis_index("row")
    rows = ids_ref.shape[0]
    cols = out_ref.shape[0] // rows
    fetches[0].wait()
    fetches[1].wait()
    mine = book_ref[pl.ds(u, 12, stride=8), :]
    for r in range(rows):
        half = mine[(r % 2) * 6 : (r % 2) * 6 + 6, :]
        ids = ids_ref[r : r + 1, :].astype(jnp.float32)
        tile = jnp.concatenate([half, ids, ids], axis=0)
        out_ref[r * cols : (r + 1) * cols] = jnp.broadcast_to(tile[None], (cols, 8, LANES))
    send = pltpu.make_async_copy(out_ref, out_hbm, sems.at[3])
    send.start()
    fetches[2].wait()
    send.wait()


def pinned(x):
    return pltpu.with_memory_space_constraint(x, pltpu.HBM)


def local(vectors, list_ids, pq_codes, fill_counts, centroids, codebook):
    row_count = lax.axis_size("row")
    col_count = lax.axis_size("col")
    devices = row_count * col_count
    slots, width = vectors.shape
    cap = slots // devices
    subs = pq_codes.shape[1]
    f32 = jnp.float32
    my_row = lax.axis_index("row")
    core = my_row % 2

    per_row = LANES // cap
    vmem = pl.BlockSpec(memory_space=pltpu.VMEM)
    smem = pl.BlockSpec(memory_space=pltpu.SMEM)
    hbm = pl.BlockSpec(memory_space=pltpu.HBM)
    sent, lists = pl.pallas_call(
        pack_kernel,
        in_specs=[hbm, hbm, hbm],
        out_specs=[hbm, vmem],
        out_shape=[
            pltpu.HBM((devices, 8, LANES), f32),
            pltpu.VMEM((centroids.size // LANES, LANES), f32),
        ],
        scratch_shapes=[
            pltpu.VMEM((row_count, LANES), jnp.int32),
            pltpu.VMEM((codebook.size // LANES, LANES), f32),
            pltpu.VMEM((devices, 8, LANES), f32),
            pltpu.SemaphoreType.DMA((4,)),
        ],
        compiler_params=pltpu.CompilerParams(vmem_limit_bytes=4 << 20),
        name="pack",
    )(
        pinned(list_ids.reshape(row_count, LANES)),
        pinned(tiled_view(codebook.reshape(-1, codebook.shape[2]))),
        pinned(tiled_view(centroids)),
    )
    got = lax.all_to_all(sent, BOTH, 0, 0, tiled=True)
    sibling = lax.ppermute(got, "row", [(i, i ^ 1) for i in range(row_count)])

    me = my_row * col_count + lax.axis_index("col")
    want = lax.dynamic_slice(got[:, 6], (0, (me % per_row) * cap), (devices, cap))
    want = want.astype(jnp.int32).reshape(slots) % centroids.shape[0]
    start = (want // 8) * (8 * width // LANES) + want % 8
    picked = pl.pallas_call(
        pick_kernel,
        in_specs=[smem, vmem],
        out_specs=hbm,
        out_shape=pltpu.HBM((slots * width // LANES, LANES), f32),
        scratch_shapes=[pltpu.VMEM((slots * width // LANES, LANES), f32), pltpu.SemaphoreType.DMA((PARTS,))],
        compiler_params=pltpu.CompilerParams(vmem_limit_bytes=8 << 20),
        name="pick",
    )(start, lists)
    picked = untiled_view(picked, slots, width)
    cent = lax.all_to_all(picked.reshape(devices, cap, width), BOTH, 0, 0, tiled=True)
    cent = tiled_view(cent.reshape(slots, width))

    view = (slots * width // LANES, LANES)
    book = (subs // 2, 256, LANES)
    vt, w, a, rows, pos, live = pl.pallas_call(
        prep_kernel,
        in_specs=[smem, smem, vmem, vmem, vmem, vmem, vmem],
        out_specs=[hbm] * 4 + [vmem] * 2,
        out_shape=[
            pltpu.HBM((width, slots), f32),
            pltpu.HBM(view, f32),
            pltpu.HBM(book, jnp.bfloat16),
            pltpu.HBM((slots,), jnp.int32),
            jax.ShapeDtypeStruct((slots // LANES, LANES), jnp.int32),
            jax.ShapeDtypeStruct((slots // LANES, LANES), jnp.int32),
        ],
        scratch_shapes=[
            pltpu.SMEM((slots,), jnp.int32),
            pltpu.VMEM((width, slots), f32),
            pltpu.VMEM(view, f32),
            pltpu.VMEM(book, jnp.bfloat16),
            pltpu.VMEM((view[0] // 2, LANES), f32),
            pltpu.SemaphoreType.DMA((4,)),
        ],
        compiler_params=pltpu.CompilerParams(vmem_limit_bytes=32 << 20),
        name="prep",
    )(
        core.reshape(1).astype(jnp.int32),
        fill_counts[0],
        fill_counts,
        tiled_view(vectors),
        pq_codes.T,
        got.reshape(devices * 8, LANES),
        sibling.reshape(devices * 8, LANES),
    )

    coded, best = pl.pallas_call(
        score_kernel,
        in_specs=[hbm, hbm, hbm, vmem, hbm, vmem, vmem],
        out_specs=[vmem] * 2,
        out_shape=[jax.ShapeDtypeStruct((slots // LANES, LANES), f32)] * 2,
        scratch_shapes=[
            pltpu.SMEM((slots,), jnp.int32),
            pltpu.VMEM((width, slots), f32),
            pltpu.VMEM(view, f32),
            pltpu.VMEM(book, jnp.bfloat16),
            pltpu.VMEM((view[0] // 4, LANES), f32),
            pltpu.VMEM((16, slots), f32),
            pltpu.VMEM((slots, LANES), f32),
            pltpu.SemaphoreType.DMA((len(STAGES), 3)),
        ],
        compiler_params=pltpu.CompilerParams(vmem_limit_bytes=32 << 20),
        name="score",
    )(pinned(rows), pinned(vt), pinned(w), cent, pinned(a), pos, live)
    return coded.reshape(slots), best.reshape(slots)


def solution(mesh):
    in_specs = (
        P(BOTH, None),
        P(BOTH),
        P(BOTH, None),
        P(BOTH, None),
        P(BOTH, None),
        P("col", None, None),
    )
    out_specs = (P(BOTH), P(BOTH))
    return jax.shard_map(local, mesh=mesh, in_specs=in_specs, out_specs=out_specs, check_vma=False)
```

```python
import jax
import jax.numpy as jnp
from jax import lax
from jax.experimental import pallas as pl
from jax.experimental.pallas import tpu as pltpu
from jax.sharding import PartitionSpec as P

BOTH = ("row", "col")
LANES = 128
SPLITS = 64


def three_way(x):
    hi = x.astype(jnp.bfloat16).astype(jnp.float32)
    rest = x - hi
    mid = rest.astype(jnp.bfloat16).astype(jnp.float32)
    lo = (rest - mid).astype(jnp.bfloat16).astype(jnp.float32)
    return hi, mid, lo


KEPT = 4


def head_rows(ref, first, block):
    tiles = 6
    top = lax.broadcasted_iota(jnp.int32, (8, LANES), 0) < KEPT
    rows = []
    for e in range(16):
        at = (first + 2 * e) * 8 * tiles + block * 8
        even, odd = ref[at : at + 8, :], ref[at + 8 * tiles : at + 8 * tiles + 8, :]
        rows.append(jnp.where(top, even, pltpu.roll(odd, KEPT, axis=0)))
    return jnp.concatenate(rows, axis=0)


def tail_rows(ref, first, block):
    tiles = 6
    spots = [(first // 8 + e) * 8 * tiles + block * 8 for e in range(16)]
    return jnp.concatenate([ref[at : at + 8, :] for at in spots], axis=0)


def prep_kernel(
    core_ref, fill_ref, fills_ref, vec_ref, codes_ref, own_ref, sib_ref, vt_hbm, w_hbm, a_hbm, list_hbm, pos_ref, live_ref,
    list_ref, vt_ref, w_ref, a_ref, tail_ref, sems
):
    core = core_ref[0]
    tiles = 6
    pairs = fill_ref.shape[0]
    rows = pairs * 8
    tail = rows // 2
    sublane = lax.broadcasted_iota(jnp.int32, (8, 256), 0)

    def no_row(i, carry):
        list_ref[i] = 0
        return carry

    def one_pair(d, at):
        for j in range(KEPT, 8):
            list_ref[at + j - KEPT] = d * (8 * tiles) + j
        return at + jnp.maximum(fill_ref[d] - KEPT, 0)

    lax.fori_loop(0, tail, no_row, 0)
    list_ref[list_ref.shape[0] - 1] = lax.fori_loop(0, pairs, one_pair, 0)
    sent = [pltpu.make_async_copy(list_ref, list_hbm, sems.at[3])]
    sent[0].start()

    across = lax.broadcasted_iota(jnp.int32, (pairs, pairs), 1)
    down = lax.broadcasted_iota(jnp.int32, (pairs, pairs), 0)
    spot = lax.broadcasted_iota(jnp.int32, pos_ref.shape, 0) * LANES + lax.broadcasted_iota(jnp.int32, pos_ref.shape, 1)
    slot = spot % 8
    fills = jnp.broadcast_to(fills_ref[...], pos_ref.shape)
    extra = jnp.maximum(fills - KEPT, 0).astype(jnp.float32).astype(jnp.bfloat16)
    earlier = jnp.where(down < across, 1.0, 0.0).astype(jnp.bfloat16)
    before = jnp.dot(extra, earlier, preferred_element_type=jnp.float32).astype(jnp.int32)
    fill_of = jnp.take_along_axis(fills, spot // 8, axis=1, mode="promise_in_bounds")
    before_of = jnp.take_along_axis(before, spot // 8, axis=1, mode="promise_in_bounds")
    pos_ref[...] = jnp.where(slot < KEPT, KEPT * (spot // 8) + slot, tail + before_of + slot - KEPT)
    live_ref[...] = (slot < fill_of).astype(jnp.int32)

    def some(i, carry):
        for k in range(32):
            row = vec_ref[pl.ds(list_ref[i * 32 + k], tiles, stride=8), :]
            tail_ref[pl.ds((i * 4 + k // 8) * (8 * tiles) + k % 8, tiles, stride=8), :] = row
        return carry

    lax.fori_loop(0, tail // 32, some, 0)
    for block in range(tiles):
        feats = slice(block * LANES, (block + 1) * LANES)
        for g in range(tail // LANES):
            vt_ref[feats, g * LANES : (g + 1) * LANES] = head_rows(vec_ref, g * 32, block).T
            vt_ref[feats, tail + g * LANES : tail + (g + 1) * LANES] = tail_rows(tail_ref, g * LANES, block).T
    sent.append(pltpu.make_async_copy(vt_ref, vt_hbm, sems.at[0]))
    sent[1].start()

    def one_block(block, carry):
        codes = codes_ref[pl.ds(pl.multiple_of(block * 16, 16), 16), :]
        stack = []
        words_of = []
        for i in range(16):
            m = block * 16 + i
            shard, within = m // 6, m % 6
            half, j = within // 3, within % 3
            base = shard * 8 + j * 2
            mine = half == core
            words = []
            for h in range(2):
                spot = pl.ds(base + h, 8, stride=LANES)
                words.append(jnp.where(mine, own_ref[spot, :], sib_ref[spot, :]))
            words_of.append(words)
            both = jnp.concatenate(words, axis=1)
            norm = jnp.sum(both * both, axis=0, keepdims=True)
            hi, mid, lo = three_way(-2.0 * both)
            nhi, nmid, nlo = three_way(norm)
            norms = jnp.where(sublane == 0, nhi, jnp.where(sublane == 1, nmid, jnp.where(sublane == 2, nlo, 0.0)))
            stack += [hi, hi, hi, mid, mid, lo, norms, jnp.zeros_like(norms)]
            if i % 2 == 1:
                a_ref[m // 2] = jnp.concatenate(stack, axis=0).T.astype(jnp.bfloat16)
                stack = []
        for g in range(rows // LANES):
            cut = slice(g * LANES, (g + 1) * LANES)
            coded = []
            for i in range(16):
                code = jnp.broadcast_to(codes[i : i + 1, cut], (8, LANES))
                low = code & (LANES - 1)
                first = jnp.take_along_axis(words_of[i][0], low, axis=1, mode="promise_in_bounds")
                second = jnp.take_along_axis(words_of[i][1], low, axis=1, mode="promise_in_bounds")
                coded.append(jnp.where(code >= LANES, second, first))
            turned = jnp.concatenate(coded, axis=0).T
            for e in range(16):
                at = pl.ds(pl.multiple_of((g * 16 + e) * (8 * tiles) + block * 8, 8), 8)
                w_ref[at, :] = vec_ref[at, :] - turned[e * 8 : (e + 1) * 8, :]
        return carry

    lax.fori_loop(0, tiles, one_block, 0)
    sent += [
        pltpu.make_async_copy(w_ref, w_hbm, sems.at[1]),
        pltpu.make_async_copy(a_ref, a_hbm, sems.at[2]),
    ]
    for copy in sent[2:]:
        copy.start()
    for copy in sent:
        copy.wait()


PARTS = 8


def pick_kernel(start_ref, cent_ref, out_hbm, out_ref, sems):
    tiles = 6
    words = out_ref.shape[0] // PARTS
    slots = words // tiles
    copies = []
    for part in range(PARTS):
        for k in range(slots):
            row = cent_ref[pl.ds(start_ref[part * slots + k], tiles, stride=8), :]
            out_ref[pl.ds(part * words + k // 8 * (8 * tiles) + k % 8, tiles, stride=8), :] = row
        cut = slice(part * words, (part + 1) * words)
        copies.append(pltpu.make_async_copy(out_ref.at[cut], out_hbm.at[cut], sems.at[part]))
        copies[-1].start()
    for copy in copies:
        copy.wait()


def tiled_view(x):
    n, w = x.shape
    return x.reshape(n // 8, 8, w // LANES, LANES).swapaxes(1, 2).reshape(n * w // LANES, LANES)


def untiled_view(x, n, w):
    return x.reshape(n // 8, w // LANES, 8, LANES).swapaxes(1, 2).reshape(n, w)


STAGES = ((0, 1), (1, 3), (3, 6))


def score_kernel(
    list_hbm, vt_hbm, w_hbm, cent_ref, a_hbm, pos_ref, live_ref, coded_ref, best_ref,
    list_ref, vt_ref, w_ref, a_ref, tail_ref, acc_ref, part_ref, sems
):
    tiles = 6
    rows = pos_ref.shape[0] * LANES
    wide = 256
    head = rows // 2
    sure = slice(0, head + wide)

    def fetch(k):
        lo, hi = STAGES[k]
        pairs, feats = slice(lo * 8, hi * 8), slice(lo * LANES, hi * LANES)
        copies = [
            pltpu.make_async_copy(a_hbm.at[pairs], a_ref.at[pairs], sems.at[k, 0]),
            pltpu.make_async_copy(vt_hbm.at[feats, sure], vt_ref.at[feats, sure], sems.at[k, 1]),
        ]
        if hi == tiles:
            copies.append(pltpu.make_async_copy(w_hbm, w_ref, sems.at[k, 2]))
        for copy in copies:
            copy.start()
        return copies

    def gather(first):
        for k in range(wide):
            row = cent_ref[pl.ds(list_ref[first + k], tiles, stride=8), :]
            tail_ref[pl.ds(k // 8 * (8 * tiles) + k % 8, tiles, stride=8), :] = row

    ones = jnp.ones((16, wide), jnp.bfloat16)
    none = jnp.zeros((SPLITS, wide), jnp.bfloat16)

    def score(block, t):
        cut = slice(t * wide, (t + 1) * wide)
        if t * wide < head:
            cent = [head_rows(cent_ref, t * 64 + g * 32, block).T for g in range(2)]
        else:
            cent = [tail_rows(tail_ref, g * LANES, block).T for g in range(2)]
        resid = vt_ref[block * LANES : (block + 1) * LANES, cut] - jnp.concatenate(cent, axis=1)
        least = jnp.zeros((1, wide), jnp.float32)
        for pair in range(8):
            left = a_ref[block * 8 + pair]
            for half in range(2):
                at = (pair * 2 + half) * 8
                top, mid, low = three_way(resid[at : at + 8, :])
                side = [
                    jnp.concatenate([top, mid], axis=0).astype(jnp.bfloat16),
                    jnp.concatenate([low, top], axis=0).astype(jnp.bfloat16),
                    jnp.concatenate([mid, top], axis=0).astype(jnp.bfloat16),
                    ones,
                ]
                side = [none] + side if half else side + [none]
                table = jnp.dot(left, jnp.concatenate(side, axis=0), preferred_element_type=jnp.float32)
                least += jnp.min(table, axis=0, keepdims=True)
        acc_ref[0:8, cut] += jnp.sum((resid * resid).reshape(16, 8, wide), axis=0)
        acc_ref[8:9, cut] += least

    order = pltpu.make_async_copy(list_hbm, list_ref, sems.at[0, 2])
    order.start()
    waiting = fetch(0)
    acc_ref[...] = jnp.zeros_like(acc_ref)
    order.wait()
    gather(0)
    for k, (lo, hi) in enumerate(STAGES):
        for copy in waiting:
            copy.wait()
        if k + 1 < len(STAGES):
            waiting = fetch(k + 1)
        for block in range(lo, hi):
            for t in range(3):
                score(block, t)
            if hi == tiles:
                share = rows // 8 // (hi - lo) + 1
                for d in range((block - lo) * share, min((block - lo + 1) * share, rows // 8)):
                    total = jnp.zeros((8, LANES), jnp.float32)
                    for b in range(tiles):
                        at = slice((d * tiles + b) * 8, (d * tiles + b + 1) * 8)
                        err = w_ref[at, :] - cent_ref[at, :]
                        total += err * err
                    part_ref[d * 8 : (d + 1) * 8, :] = total

    live = live_ref[...] != 0
    coded = [
        jnp.sum(part_ref[h * LANES : (h + 1) * LANES, :].T, axis=0, keepdims=True) for h in range(rows // LANES)
    ]
    coded_ref[...] = jnp.where(live, jnp.concatenate(coded, axis=0), 0.0)

    @pl.when(list_ref[list_ref.shape[0] - 1] > wide)
    def _():
        rest = slice(sure.stop, rows)
        last = pltpu.make_async_copy(vt_hbm.at[:, rest], vt_ref.at[:, rest], sems.at[0, 0])
        last.start()
        gather(wide)
        last.wait()
        for block in range(tiles):
            score(block, 3)

    best = jnp.sum(acc_ref[0:8, :], axis=0, keepdims=True) + acc_ref[8:9, :]
    pos = pos_ref[...]
    found = jnp.zeros(pos.shape, jnp.float32)
    for h in range(rows // LANES):
        source = jnp.broadcast_to(best[:, h * LANES : (h + 1) * LANES], pos.shape)
        lane = jnp.take_along_axis(source, pos & (LANES - 1), axis=1, mode="promise_in_bounds")
        found = jnp.where(pos // LANES == h, lane, found)
    best_ref[...] = jnp.where(live_ref[...] != 0, found, 0.0)


def pack_kernel(ids_hbm, book_hbm, lists_hbm, out_hbm, lists_ref, ids_ref, book_ref, out_ref, sems):
    fetches = [
        pltpu.make_async_copy(book_hbm, book_ref, sems.at[0]),
        pltpu.make_async_copy(ids_hbm, ids_ref, sems.at[1]),
        pltpu.make_async_copy(lists_hbm, lists_ref, sems.at[2]),
    ]
    for fetch in fetches:
        fetch.start()
    u = lax.axis_index("row")
    rows = ids_ref.shape[0]
    cols = out_ref.shape[0] // rows
    fetches[0].wait()
    fetches[1].wait()
    mine = book_ref[pl.ds(u, 12, stride=8), :]
    for r in range(rows):
        half = mine[(r % 2) * 6 : (r % 2) * 6 + 6, :]
        ids = ids_ref[r : r + 1, :].astype(jnp.float32)
        tile = jnp.concatenate([half, ids, ids], axis=0)
        out_ref[r * cols : (r + 1) * cols] = jnp.broadcast_to(tile[None], (cols, 8, LANES))
    send = pltpu.make_async_copy(out_ref, out_hbm, sems.at[3])
    send.start()
    fetches[2].wait()
    send.wait()


def pinned(x):
    return pltpu.with_memory_space_constraint(x, pltpu.HBM)


def local(vectors, list_ids, pq_codes, fill_counts, centroids, codebook):
    row_count = lax.axis_size("row")
    col_count = lax.axis_size("col")
    devices = row_count * col_count
    slots, width = vectors.shape
    cap = slots // devices
    subs = pq_codes.shape[1]
    f32 = jnp.float32
    my_row = lax.axis_index("row")
    core = my_row % 2

    per_row = LANES // cap
    vmem = pl.BlockSpec(memory_space=pltpu.VMEM)
    smem = pl.BlockSpec(memory_space=pltpu.SMEM)
    hbm = pl.BlockSpec(memory_space=pltpu.HBM)
    sent, lists = pl.pallas_call(
        pack_kernel,
        in_specs=[hbm, hbm, hbm],
        out_specs=[hbm, vmem],
        out_shape=[
            pltpu.HBM((devices, 8, LANES), f32),
            pltpu.VMEM((centroids.size // LANES, LANES), f32),
        ],
        scratch_shapes=[
            pltpu.VMEM((row_count, LANES), jnp.int32),
            pltpu.VMEM((codebook.size // LANES, LANES), f32),
            pltpu.VMEM((devices, 8, LANES), f32),
            pltpu.SemaphoreType.DMA((4,)),
        ],
        compiler_params=pltpu.CompilerParams(vmem_limit_bytes=4 << 20),
        name="pack",
    )(
        pinned(list_ids.reshape(row_count, LANES)),
        pinned(tiled_view(codebook.reshape(-1, codebook.shape[2]))),
        pinned(tiled_view(centroids)),
    )
    got = lax.all_to_all(sent, BOTH, 0, 0, tiled=True)
    sibling = lax.ppermute(got, "row", [(i, i ^ 1) for i in range(row_count)])

    me = my_row * col_count + lax.axis_index("col")
    want = lax.dynamic_slice(got[:, 6], (0, (me % per_row) * cap), (devices, cap))
    want = want.astype(jnp.int32).reshape(slots) % centroids.shape[0]
    start = (want // 8) * (8 * width // LANES) + want % 8
    picked = pl.pallas_call(
        pick_kernel,
        in_specs=[smem, vmem],
        out_specs=hbm,
        out_shape=pltpu.HBM((slots * width // LANES, LANES), f32),
        scratch_shapes=[pltpu.VMEM((slots * width // LANES, LANES), f32), pltpu.SemaphoreType.DMA((PARTS,))],
        compiler_params=pltpu.CompilerParams(vmem_limit_bytes=8 << 20),
        name="pick",
    )(start, lists)
    picked = untiled_view(picked, slots, width)
    cent = lax.all_to_all(picked.reshape(devices, cap, width), BOTH, 0, 0, tiled=True)
    cent = tiled_view(cent.reshape(slots, width))

    view = (slots * width // LANES, LANES)
    book = (subs // 2, 256, LANES)
    vt, w, a, rows, pos, live = pl.pallas_call(
        prep_kernel,
        in_specs=[smem, smem, vmem, vmem, vmem, vmem, vmem],
        out_specs=[hbm] * 4 + [vmem] * 2,
        out_shape=[
            pltpu.HBM((width, slots), f32),
            pltpu.HBM(view, f32),
            pltpu.HBM(book, jnp.bfloat16),
            pltpu.HBM((slots,), jnp.int32),
            jax.ShapeDtypeStruct((slots // LANES, LANES), jnp.int32),
            jax.ShapeDtypeStruct((slots // LANES, LANES), jnp.int32),
        ],
        scratch_shapes=[
            pltpu.SMEM((slots,), jnp.int32),
            pltpu.VMEM((width, slots), f32),
            pltpu.VMEM(view, f32),
            pltpu.VMEM(book, jnp.bfloat16),
            pltpu.VMEM((view[0] // 2, LANES), f32),
            pltpu.SemaphoreType.DMA((4,)),
        ],
        compiler_params=pltpu.CompilerParams(vmem_limit_bytes=32 << 20),
        name="prep",
    )(
        core.reshape(1).astype(jnp.int32),
        fill_counts[0],
        fill_counts,
        tiled_view(vectors),
        pq_codes.T,
        got.reshape(devices * 8, LANES),
        sibling.reshape(devices * 8, LANES),
    )

    coded, best = pl.pallas_call(
        score_kernel,
        in_specs=[hbm, hbm, hbm, vmem, hbm, vmem, vmem],
        out_specs=[vmem] * 2,
        out_shape=[jax.ShapeDtypeStruct((slots // LANES, LANES), f32)] * 2,
        scratch_shapes=[
            pltpu.SMEM((slots,), jnp.int32),
            pltpu.VMEM((width, slots), f32),
            pltpu.VMEM(view, f32),
            pltpu.VMEM(book, jnp.bfloat16),
            pltpu.VMEM((view[0] // 4, LANES), f32),
            pltpu.VMEM((16, slots), f32),
            pltpu.VMEM((slots, LANES), f32),
            pltpu.SemaphoreType.DMA((len(STAGES), 3)),
        ],
        compiler_params=pltpu.CompilerParams(vmem_limit_bytes=32 << 20),
        name="score",
    )(pinned(rows), pinned(vt), pinned(w), cent, pinned(a), pos, live)
    return coded.reshape(slots), best.reshape(slots)


def solution(mesh):
    in_specs = (
        P(BOTH, None),
        P(BOTH),
        P(BOTH, None),
        P(BOTH, None),
        P(BOTH, None),
        P("col", None, None),
    )
    out_specs = (P(BOTH), P(BOTH))
    return jax.shard_map(local, mesh=mesh, in_specs=in_specs, out_specs=out_specs, check_vma=False)
```
